128 devices in a mesh: replica: 1, dp: 128 (over z, y, x, core).
Axes of the slice: x: 4, y: 4, z: 4, core: 2. Of those that a mesh axis runs over, the one named last changes fastest.
Arguments:
- x: bfloat16 [256, 2048], P(('replica', 'dp'))
- lengths: int32 [256], P(('replica', 'dp'))
- cache: bfloat16 [2, 256, 1024, 576], P(None, ('replica', 'dp'))
- attn_gain: float32 [2, 2048], replicated
- ffn_gain: float32 [2, 2048], replicated
- w_query: bfloat16 [2, 2048, 9216], replicated
- w_attn_out: bfloat16 [2, 8192, 2048], replicated
- w_up: bfloat16 [2, 2048, 11264], P(None, None, 'dp')
- w_gate: bfloat16 [2, 2048, 11264], P(None, None, 'dp')
- w_down: bfloat16 [2, 11264, 2048], P(None, 'dp')
Outputs:
- output: bfloat16 [256, 2048], P(('replica', 'dp'))
All inputs are finite; a program needn't handle non-finite values.
Results may differ from the reference program's by a relative error of at most 0.02.
Values are sent between devices in bfloat16 or wider.
A program may use at most 1 GiB of HBM per device.

```python
import jax
import jax.numpy as jnp
from jax import lax

B_DEV = 2
GROUP_SIZE = 128
SEQ_LEN = 1024
D_MODEL = 2048
FF_DIM = 11264
HEADS = 16
LATENT = 512
ROPE = 64
LAYERS = 2

NORM_EPS = 1e-6
BATCH = B_DEV * GROUP_SIZE
KV_DIM = LATENT + ROPE
SCORE_SCALE = (3 * ROPE) ** -0.5
LEN_FLOOR = max(1, SEQ_LEN // 16)
CAP_FLOOR = max(LEN_FLOOR, SEQ_LEN // 4)


def draw_lengths(key):
    cap_key, len_key, pick_key = jax.random.split(key, 3)
    caps = jax.random.randint(cap_key, (GROUP_SIZE,), CAP_FLOOR, SEQ_LEN + 1)
    full_dev = jax.random.randint(pick_key, (), 0, GROUP_SIZE)
    caps = jnp.where(jnp.arange(GROUP_SIZE) == full_dev, SEQ_LEN, caps)
    drawn = jax.random.randint(len_key, (GROUP_SIZE, B_DEV), LEN_FLOOR, caps[:, None] + 1)
    drawn = jnp.concatenate([drawn[:, 1:], caps[:, None]], axis=1)
    return jnp.sort(drawn, axis=1).reshape(BATCH).astype(jnp.int32)


def setup_inputs(seed: int = 0, part: int = 0) -> dict:
    part_key = jax.random.fold_in(jax.random.key(seed), part)
    x_key, len_key, cache_key = jax.random.split(part_key, 3)
    shared_keys = jax.random.split(jax.random.key(seed + 1), 7)
    wo_scale = (HEADS * LATENT) ** -0.5 * max(1.0, (SEQ_LEN / 64) ** 0.5)
    return {
        'x': jax.random.normal(x_key, (BATCH, D_MODEL), jnp.float32).astype(jnp.bfloat16),
        'lengths': draw_lengths(len_key),
        'cache': jax.random.normal(cache_key, (LAYERS, BATCH, SEQ_LEN, KV_DIM), jnp.float32).astype(jnp.bfloat16),
        'attn_gain': 0.5 + jax.random.uniform(shared_keys[0], (LAYERS, D_MODEL), jnp.float32),
        'ffn_gain': 0.5 + jax.random.uniform(shared_keys[1], (LAYERS, D_MODEL), jnp.float32),
        'w_query': (jax.random.normal(shared_keys[2], (LAYERS, D_MODEL, HEADS * KV_DIM), jnp.float32) * D_MODEL ** -0.5).astype(jnp.bfloat16),
        'w_attn_out': (jax.random.normal(shared_keys[3], (LAYERS, HEADS * LATENT, D_MODEL), jnp.float32) * wo_scale).astype(jnp.bfloat16),
        'w_up': (jax.random.normal(shared_keys[4], (LAYERS, D_MODEL, FF_DIM), jnp.float32) * D_MODEL ** -0.5).astype(jnp.bfloat16),
        'w_gate': (jax.random.normal(shared_keys[5], (LAYERS, D_MODEL, FF_DIM), jnp.float32) * D_MODEL ** -0.5).astype(jnp.bfloat16),
        'w_down': (jax.random.normal(shared_keys[6], (LAYERS, FF_DIM, D_MODEL), jnp.float32) * 2.0 * FF_DIM ** -0.5).astype(jnp.bfloat16),
    }


def rms_norm(rows, gain):
    rows_f = rows.astype(jnp.float32)
    mean_sq = jnp.mean(rows_f * rows_f, axis=-1, keepdims=True)
    return (rows_f * lax.rsqrt(mean_sq + NORM_EPS) * gain).astype(jnp.bfloat16)


def attention_layer(x_all, lengths, cache_l, gain, wq_l, wo_l):
    x_blocks = x_all.reshape(GROUP_SIZE, B_DEV, D_MODEL)
    len_blocks = lengths.reshape(GROUP_SIZE, B_DEV)
    cache_blocks = cache_l.reshape(GROUP_SIZE, B_DEV, SEQ_LEN, KV_DIM)
    positions = jnp.arange(SEQ_LEN)[None, None, :]

    def one_block(block):
        x_rows, len_rows, cache_rows = block
        normed = rms_norm(x_rows, gain)
        query = jnp.dot(normed, wq_l, preferred_element_type=jnp.float32).astype(jnp.bfloat16)
        query = query.reshape(B_DEV, HEADS, KV_DIM).astype(jnp.float32)
        cache_f = cache_rows.astype(jnp.float32)
        scores = jnp.einsum('bhc,btc->bht', query, cache_f) * SCORE_SCALE
        scores = jnp.where(positions < len_rows[:, None, None], scores, -jnp.inf)
        attn_probs = jax.nn.softmax(scores, axis=-1).astype(jnp.bfloat16).astype(jnp.float32)
        mixed = jnp.einsum('bht,btc->bhc', attn_probs, cache_f[:, :, :LATENT]).astype(jnp.bfloat16)
        attn_out = jnp.dot(mixed.reshape(B_DEV, HEADS * LATENT), wo_l, preferred_element_type=jnp.float32)
        return (x_rows.astype(jnp.float32) + attn_out).astype(jnp.bfloat16)

    return lax.map(one_block, (x_blocks, len_blocks, cache_blocks)).reshape(BATCH, D_MODEL)


def ffn_layer(x_all, gain, wu_l, wg_l, wd_l):
    normed = rms_norm(x_all, gain)
    gate_pre = jnp.dot(normed, wg_l, preferred_element_type=jnp.float32)
    up_pre = jnp.dot(normed, wu_l, preferred_element_type=jnp.float32)
    hidden = (jax.nn.silu(gate_pre) * up_pre).astype(jnp.bfloat16)
    ffn_out = jnp.dot(hidden, wd_l, preferred_element_type=jnp.float32)
    return (x_all.astype(jnp.float32) + ffn_out).astype(jnp.bfloat16)


def reference(x, lengths, cache, attn_gain, ffn_gain, w_query, w_attn_out, w_up, w_gate, w_down):
    def layer_step(x_cur, params):
        cache_l, gain_a, gain_f, wq_l, wo_l, wu_l, wg_l, wd_l = params
        x_cur = attention_layer(x_cur, lengths, cache_l, gain_a, wq_l, wo_l)
        x_cur = ffn_layer(x_cur, gain_f, wu_l, wg_l, wd_l)
        return x_cur, None

    x_final, _ = lax.scan(layer_step, x, (cache, attn_gain, ffn_gain, w_query, w_attn_out, w_up, w_gate, w_down))
    return x_final
```

```python
import functools

import jax
import jax.numpy as jnp
from jax import lax
from jax.experimental import pallas as pl
from jax.experimental.pallas import tpu as pltpu
from jax.sharding import PartitionSpec as P

NORM_EPS = 1e-6
MESH = pl.DeviceIdType.MESH
F32 = jnp.float32
BF16 = jnp.bfloat16


def dot(a, b):
    return jnp.dot(a, b, preferred_element_type=F32)


def dot_nt(a, b):
    return lax.dot_general(a, b, (((1,), (1,)), ((), ())), preferred_element_type=F32)


def kernel(
    cfg,
    x_ref, len_ref, ag_ref, fg_ref, cache_hbm, wq_hbm, wo_hbm, wu_hbm, wg_hbm, wd_hbm,
    out_ref,
    wq, wo, cbuf, wu, wg, wd,
    xsend, xrecv, qrow, qsend, qbuf, obuf, osend, orecv, lhs, ysend, yrecv, xh,
    p1, ga, gb, dsend, drecv, sa, sb, r1a, r1b, ta, tb, r2a, r2b, u3, r3,
    wq_sem, wo_sem, c_sem, f_sem, ssem, rsem,
):
    side, layers, heads, kv, latent, seq, d_model, q_chunk = cfg
    half, quarter = d_model // 2, d_model // 4
    heads_half = heads // 2
    qw = heads_half * kv
    n_q = qw // q_chunk
    scale = (3 * (kv - latent)) ** -0.5

    me = lax.axis_index('dp')
    core = lax.rem(me, 2)
    chip = lax.div(me, 2)
    cx = lax.rem(chip, side)
    cy = lax.rem(lax.div(chip, side), side)
    cz = lax.div(chip, side * side)
    other = 1 - core

    def device(z, y, x, k):
        return {'dp': ((z * side + y) * side + x) * 2 + k}

    def step(c, d):
        return lax.rem(c + d, side)

    partner = device(cz, cy, cx, other)
    x_peer = {d: device(cz, cy, step(cx, d), core) for d in range(1, side)}
    y_peer = {d: device(cz, step(cy, d), cx, core) for d in range(1, side)}
    z_peer = {d: device(step(cz, d), cy, cx, core) for d in range(1, side)}

    def wq_copy(layer, i):
        cols = pl.ds(pl.multiple_of(core * qw + i * q_chunk, 128), q_chunk)
        return pltpu.make_async_copy(wq_hbm.at[layer, :, cols], wq.at[i], wq_sem.at[i])

    def wo_copy(layer, i):
        rows = pl.ds(pl.multiple_of((core * heads_half + i) * latent, 128), latent)
        return pltpu.make_async_copy(wo_hbm.at[layer, rows, :], wo.at[i], wo_sem.at[i])

    def cache_copy(layer, b):
        return pltpu.make_async_copy(cache_hbm.at[layer, b], cbuf.at[b], c_sem.at[b])

    def ffn_copies(layer):
        return [
            pltpu.make_async_copy(wg_hbm.at[layer], wg.at[layer], f_sem.at[layer, 0]),
            pltpu.make_async_copy(wu_hbm.at[layer], wu.at[layer], f_sem.at[layer, 1]),
            pltpu.make_async_copy(wd_hbm.at[layer], wd.at[layer], f_sem.at[layer, 2]),
        ]

    for i in range(n_q):
        wq_copy(0, i).start()
    for b in range(2):
        cache_copy(0, b).start()
    for i in range(heads_half):
        wo_copy(0, i).start()
    for layer in range(layers):
        for copy in ffn_copies(layer):
            copy.start()

    barrier = pltpu.get_barrier_semaphore()
    peers = [partner, *x_peer.values(), *y_peer.values(), *z_peer.values()]
    for peer in peers:
        pl.semaphore_signal(barrier, inc=1, device_id=peer, device_id_type=MESH)
    pl.semaphore_wait(barrier, len(peers))

    lhs[:, 4:8, :] = jnp.zeros((heads_half, 4, latent), F32)
    pending = []

    def remote(layer, index, src, dst, peer):
        return pltpu.make_async_remote_copy(
            src_ref=src, dst_ref=dst, send_sem=ssem.at[layer, index], recv_sem=rsem.at[layer, index],
            device_id=peer, device_id_type=MESH)

    def send(layer, index, src, dst, peer):
        copy = remote(layer, index, src, dst, peer)
        copy.start()
        pending.append(copy)

    def recv(layer, index, dst, peer):
        remote(layer, index, dst, dst, peer).wait_recv()

    def rms(rows, gain):
        mean_sq = jnp.mean(rows * rows, axis=-1, keepdims=True)
        return rows * lax.rsqrt(mean_sq + NORM_EPS) * gain

    def swap(rows):
        return jnp.concatenate([rows[2:4], rows[0:2]], axis=0)

    def attention(layer, x4):
        normed = rms(x4, ag_ref[layer:layer + 1, :])
        h8 = jnp.concatenate([normed, normed], axis=0).astype(BF16)

        def q_step(i, carry):
            wq_copy(layer, i).wait()
            qrow[:, pl.ds(pl.multiple_of(i * q_chunk, 128), q_chunk)] = dot(h8, wq[i])
            return carry

        lax.fori_loop(0, n_q, q_step, 0)
        if layer + 1 < layers:
            for i in range(n_q):
                wq_copy(layer + 1, i).start()
        pair = 2 * kv
        for j in range(heads_half // 2):
            block = qrow[:, j * pair:(j + 1) * pair]
            odd = pltpu.roll(block[:, latent:latent + 640], 640 - 64, 1)
            for parity, q8 in ((0, block[:, :640]), (1, odd)):
                h = 2 * j + parity
                for b in range(2):
                    qbuf[layer, core, b, h:h + 1, :] = q8[b:b + 1, :]
                    qsend[layer, b, h:h + 1, :] = q8[2 + b:3 + b, :]
        send(layer, 1, qsend.at[layer], qbuf.at[layer, core], partner)
        recv(layer, 1, qbuf.at[layer, other], partner)

        for b in range(2):
            cache_copy(layer, b).wait()
            q = jnp.concatenate([qbuf[layer, 0, b], qbuf[layer, 1, b]], axis=0)[:, :kv].astype(BF16)
            s = dot(q, cbuf[b]) * scale
            positions = lax.broadcasted_iota(jnp.int32, (heads, seq), 1)
            s = jnp.where(positions < len_ref[b], s, -jnp.inf)
            e = jnp.exp(s - jnp.max(s, axis=-1, keepdims=True))
            p = (e / jnp.sum(e, axis=-1, keepdims=True)).astype(BF16)
            o = dot_nt(p, cbuf[b, :latent, :])
            obuf[b, 0] = o[:heads_half]
            obuf[b, 1] = o[heads_half:]
        if layer + 1 < layers:
            for b in range(2):
                cache_copy(layer + 1, b).start()
        for b in range(2):
            mine = obuf[b, core]
            theirs = obuf[b, other]
            for h in range(heads_half):
                lhs[h, b:b + 1, :] = mine[h:h + 1, :]
                osend[layer, h, b:b + 1, :] = theirs[h:h + 1, :]
        send(layer, 2, osend.at[layer], orecv.at[layer], partner)
        recv(layer, 2, orecv.at[layer], partner)
        for h in range(heads_half):
            lhs[h, 2:4, :] = orecv[layer, h]

        def o_step(i, acc):
            wo_copy(layer, i).wait()
            return acc + dot(lhs[i].astype(BF16), wo[i])

        acc = lax.fori_loop(0, heads_half, o_step, jnp.zeros((8, d_model), F32))
        if layer + 1 < layers:
            for i in range(heads_half):
                wo_copy(layer + 1, i).start()
        y4 = acc[0:4]
        ysend[layer] = y4
        send(layer, 3, ysend.at[layer], yrecv.at[layer], partner)
        recv(layer, 3, yrecv.at[layer], partner)
        return (x4 + (y4 + swap(yrecv[layer]))).astype(BF16).astype(F32)

    def ffn(layer, x4):
        g4 = rms(x4, fg_ref[layer:layer + 1, :]).astype(BF16)
        p1[layer, cx] = jnp.where(core == 0, g4[:, :half], g4[:, half:])
        for d in range(1, side):
            send(layer, 4 + d, p1.at[layer, cx], p1.at[layer, cx], x_peer[d])
        for d in range(1, side):
            recv(layer, 4 + d, p1.at[layer, step(cx, side - d)], x_peer[d])
        block = jnp.concatenate([p1[layer, i].astype(F32) for i in range(side)], axis=0).astype(BF16)
        ga[layer, core, cz, cy] = block[:, :quarter]
        gb[layer, core, cz, cy] = block[:, quarter:]
        for d in range(1, side):
            send(layer, 7 + d, ga.at[layer, core, cz, cy], ga.at[layer, core, cz, cy], y_peer[d])
        for d in range(1, side):
            send(layer, 10 + d, gb.at[layer, core, cz, cy], gb.at[layer, core, cz, cy], z_peer[d])
        for d in range(1, side):
            recv(layer, 7 + d, ga.at[layer, core, cz, step(cy, side - d)], y_peer[d])
        own_a = ga.at[layer, core, cz]
        for d in range(1, side):
            send(layer, 13 + d, own_a, own_a, z_peer[d])
        send(layer, 20, own_a, own_a, partner)
        for d in range(1, side):
            recv(layer, 10 + d, gb.at[layer, core, step(cz, side - d), cy], z_peer[d])
        own_b = gb.at[layer, core, :, cy]
        for d in range(1, side):
            send(layer, 16 + d, own_b, own_b, y_peer[d])
        send(layer, 24, own_b, own_b, partner)
        for d in range(1, side):
            got_a = ga.at[layer, core, step(cz, side - d)]
            recv(layer, 13 + d, got_a, z_peer[d])
            send(layer, 20 + d, got_a, got_a, partner)
            got_b = gb.at[layer, core, :, step(cy, side - d)]
            recv(layer, 16 + d, got_b, y_peer[d])
            send(layer, 24 + d, got_b, got_b, partner)
        for copy in ffn_copies(layer):
            copy.wait()

        rows = 4 * side ** 3

        def product(w, k):
            part_a = ga[layer, k].reshape(rows, quarter)
            part_b = gb[layer, k].reshape(rows, quarter)
            base = pl.multiple_of(k * half, 128)
            w_a = w[layer, :, pl.ds(base, quarter)]
            w_b = w[layer, :, pl.ds(base + quarter, quarter)]
            return dot_nt(part_a, w_a) + dot_nt(part_b, w_b)

        gate = product(wg, core)
        up = product(wu, core)
        for d in range(side):
            recv(layer, 20 + d, ga.at[layer, other, step(cz, side - d)], partner)
            recv(layer, 24 + d, gb.at[layer, other, :, step(cy, side - d)], partner)
        gate = gate + product(wg, other)
        up = up + product(wu, other)
        hidden = (jax.nn.silu(gate) * up).astype(BF16)

        shape = (side, side, 4 * side, quarter)
        for c in range(2):
            cols = pl.ds(pl.multiple_of(other * half + c * quarter, 128), quarter)
            dsend[layer, c] = dot(hidden, wd[layer, :, cols]).reshape(shape)
            send(layer, 28 + c, dsend.at[layer, c], drecv.at[layer, c], partner)
        for c, s in ((0, sa), (1, sb)):
            cols = pl.ds(pl.multiple_of(core * half + c * quarter, 128), quarter)
            s[layer] = dot(hidden, wd[layer, :, cols]).reshape(shape)
        for c, s in ((0, sa), (1, sb)):
            recv(layer, 28 + c, drecv.at[layer, c], partner)
            s[layer] = s[layer] + drecv[layer, c]
            for d in range(1, side):
                if c == 0:
                    send(layer, 29 + d, sa.at[layer, step(cz, d)], r1a.at[layer, d - 1], z_peer[d])
                else:
                    send(layer, 32 + d, sb.at[layer, :, step(cy, d)], r1b.at[layer, d - 1], y_peer[d])
        total = sa[layer, cz]
        for d in range(1, side):
            recv(layer, 29 + d, r1a.at[layer, d - 1], z_peer[d])
            total = total + r1a[layer, d - 1]
        ta[layer] = total
        for d in range(1, side):
            send(layer, 35 + d, ta.at[layer, step(cy, d)], r2a.at[layer, d - 1], y_peer[d])
        total = sb[layer, :, cy]
        for d in range(1, side):
            recv(layer, 32 + d, r1b.at[layer, d - 1], y_peer[d])
            total = total + r1b[layer, d - 1]
        tb[layer] = total
        for d in range(1, side):
            send(layer, 38 + d, tb.at[layer, step(cz, d)], r2b.at[layer, d - 1], z_peer[d])
        total = ta[layer, cy]
        for d in range(1, side):
            recv(layer, 35 + d, r2a.at[layer, d - 1], y_peer[d])
            total = total + r2a[layer, d - 1]
        for i in range(side):
            u3[layer, i, :, :quarter] = total[4 * i:4 * i + 4]
        total = tb[layer, cz]
        for d in range(1, side):
            recv(layer, 38 + d, r2b.at[layer, d - 1], z_peer[d])
            total = total + r2b[layer, d - 1]
        for i in range(side):
            u3[layer, i, :, quarter:] = total[4 * i:4 * i + 4]
        for d in range(1, side):
            send(layer, 41 + d, u3.at[layer, step(cx, d)], r3.at[layer, d - 1], x_peer[d])
        total = u3[layer, cx]
        for d in range(1, side):
            recv(layer, 41 + d, r3.at[layer, d - 1], x_peer[d])
            total = total + r3[layer, d - 1]
        kept = jnp.where(core == 0, x4[:, :half], x4[:, half:])
        xh[layer, core] = (kept + total).astype(BF16).astype(F32)
        send(layer, 45, xh.at[layer, core], xh.at[layer, core], partner)
        recv(layer, 45, xh.at[layer, other], partner)
        return jnp.concatenate([xh[layer, 0], xh[layer, 1]], axis=1)

    def reorder(x4):
        return jnp.where(core == 0, x4, swap(x4))

    xsend[...] = x_ref[...].astype(F32)
    send(0, 0, xsend, xrecv, partner)
    recv(0, 0, xrecv, partner)
    x4 = jnp.concatenate([xsend[...], xrecv[...]], axis=0)
    for layer in range(layers):
        x4 = attention(layer, x4)
        x4 = ffn(layer, reorder(x4))
        x4 = reorder(x4)
    out_ref[...] = x4[0:2].astype(BF16)
    for copy in pending:
        copy.wait_send()


def solution(mesh):
    devices = mesh.shape['dp']
    side = round((devices // 2) ** (1 / 3))

    def local_step(x, lengths, cache, attn_gain, ffn_gain, w_query, w_attn_out, w_up, w_gate, w_down):
        layers, _, seq, kv = cache.shape
        d_model = x.shape[1]
        heads = w_query.shape[2] // kv
        latent = w_attn_out.shape[1] // heads
        hid = w_up.shape[2]
        half, quarter, hh = d_model // 2, d_model // 4, heads // 2
        q_chunk = 512
        n_q = hh * kv // q_chunk
        blk = 4 * side
        cfg = (side, layers, heads, kv, latent, seq, d_model, q_chunk)
        vmem = pl.BlockSpec(memory_space=pltpu.VMEM)
        smem = pl.BlockSpec(memory_space=pltpu.SMEM)
        hbm = pl.BlockSpec(memory_space=pl.ANY)
        scratch = [
            pltpu.VMEM((n_q, d_model, q_chunk), BF16),
            pltpu.VMEM((hh, latent, d_model), BF16),
            pltpu.VMEM((2, kv, seq), BF16),
            pltpu.VMEM((layers, hid, d_model), BF16),
            pltpu.VMEM((layers, hid, d_model), BF16),
            pltpu.VMEM((layers, hid, d_model), BF16),
            pltpu.VMEM((2, d_model), F32),
            pltpu.VMEM((2, d_model), F32),
            pltpu.VMEM((8, hh * kv), F32),
            pltpu.VMEM((layers, 2, hh, 640), F32),
            pltpu.VMEM((layers, 2, 2, hh, 640), F32),
            pltpu.VMEM((2, 2, hh, latent), F32),
            pltpu.VMEM((layers, hh, 2, latent), F32),
            pltpu.VMEM((layers, hh, 2, latent), F32),
            pltpu.VMEM((hh, 8, latent), F32),
            pltpu.VMEM((layers, 4, d_model), F32),
            pltpu.VMEM((layers, 4, d_model), F32),
            pltpu.VMEM((layers, 2, 4, half), F32),
            pltpu.VMEM((layers, side, 4, half), BF16),
            pltpu.VMEM((layers, 2, side, side, blk, quarter), BF16),
            pltpu.VMEM((layers, 2, side, side, blk, quarter), BF16),
            pltpu.VMEM((layers, 2, side, side, blk, quarter), F32),
            pltpu.VMEM((layers, 2, side, side, blk, quarter), F32),
            pltpu.VMEM((layers, side, side, blk, quarter), F32),
            pltpu.VMEM((layers, side, side, blk, quarter), F32),
            pltpu.VMEM((layers, side - 1, side, blk, quarter), F32),
            pltpu.VMEM((layers, side - 1, side, blk, quarter), F32),
            pltpu.VMEM((layers, side, blk, quarter), F32),
            pltpu.VMEM((layers, side, blk, quarter), F32),
            pltpu.VMEM((layers, side - 1, blk, quarter), F32),
            pltpu.VMEM((layers, side - 1, blk, quarter), F32),
            pltpu.VMEM((layers, side, 4, half), F32),
            pltpu.VMEM((layers, side - 1, 4, half), F32),
            pltpu.SemaphoreType.DMA((n_q,)),
            pltpu.SemaphoreType.DMA((hh,)),
            pltpu.SemaphoreType.DMA((2,)),
            pltpu.SemaphoreType.DMA((layers, 3)),
            pltpu.SemaphoreType.DMA((layers, 46)),
            pltpu.SemaphoreType.DMA((layers, 46)),
        ]
        return pl.pallas_call(
            functools.partial(kernel, cfg),
            out_shape=jax.ShapeDtypeStruct(x.shape, BF16),
            in_specs=[vmem, smem, vmem, vmem, hbm, hbm, hbm, hbm, hbm, hbm],
            out_specs=vmem,
            scratch_shapes=scratch,
            compiler_params=pltpu.CompilerParams(
                collective_id=0, has_side_effects=True, vmem_limit_bytes=66_000_000),
            name='mla_decode',
        )(x, lengths, attn_gain, ffn_gain, jnp.swapaxes(cache, 2, 3), w_query, w_attn_out,
          jnp.swapaxes(w_up, 1, 2), jnp.swapaxes(w_gate, 1, 2), w_down)

    rows = ('replica', 'dp')
    return jax.shard_map(
        local_step,
        mesh=mesh,
        in_specs=(P(rows, None), P(rows), P(None, rows, None, None), P(), P(), P(), P(),
                  P(None, None, 'dp'), P(None, None, 'dp'), P(None, 'dp', None)),
        out_specs=P(rows, None),
        check_vma=False,
    )
```

```python
import functools

import jax
import jax.numpy as jnp
from jax import lax
from jax.experimental import pallas as pl
from jax.experimental.pallas import tpu as pltpu
from jax.sharding import PartitionSpec as P

NORM_EPS = 1e-6
MESH = pl.DeviceIdType.MESH
F32 = jnp.float32
BF16 = jnp.bfloat16
COLOURS = (('z', 'y', 'x'), ('x', 'z', 'y'), ('y', 'z', 'x'))


def dot(a, b):
    return jnp.dot(a, b, preferred_element_type=F32)


def dot_nt(a, b):
    return lax.dot_general(a, b, (((1,), (1,)), ((), ())), preferred_element_type=F32)


def colour_columns(d_model):
    tiles = d_model // 128
    widths = [128 * ((tiles + 2 - c) // 3) for c in range(3)]
    return [(sum(widths[:c]), widths[c]) for c in range(3)]


def kernel(
    cfg,
    x_hbm, len_hbm, ag_hbm, fg_hbm, cache_hbm, wq_hbm, wo_hbm, wu_hbm, wg_hbm, wd_hbm,
    out_ref,
    wq, wo, cbuf, wu, wg, wd,
    xin, lens, ag, fg, lbuf, xsend, xrecv, qrow, qbuf, lhs, ysend, yrecv, asm,
    p1a, p1b, p1c, g_a, g_b, g_c, s_a, s_b, s_c, r1a, r1b, r1c, u_a, u_b, u_c, r2a, r2b, r2c,
    wq_sem, wo_sem, c_sem, f_sem, in_sem, ssem, rsem, agp_s, agp_r, rsp_s, rsp_r,
):
    side, layers, heads, kv, latent, seq, d_model, q_chunk, o_chunk = cfg
    heads_half = heads // 2
    qw = heads_half * kv
    n_q = qw // q_chunk
    n_o = d_model // o_chunk
    kdim = heads_half * latent
    plane = side * side
    rows = 2 * side ** 3
    scale = (3 * (kv - latent)) ** -0.5
    columns = colour_columns(d_model)
    p1, g_buf, s_buf = (p1a, p1b, p1c), (g_a, g_b, g_c), (s_a, s_b, s_c)
    r1, u_buf, r2 = (r1a, r1b, r1c), (u_a, u_b, u_c), (r2a, r2b, r2c)

    me = lax.axis_index('dp')
    core = lax.rem(me, 2)
    chip = lax.div(me, 2)
    coord = {'x': lax.rem(chip, side), 'y': lax.rem(lax.div(chip, side), side), 'z': lax.div(chip, plane)}
    other = 1 - core

    def step(c, d):
        return lax.rem(c + d, side)

    def device(k=core, **shift):
        at = {a: step(coord[a], shift.get(a, 0)) for a in 'zyx'}
        return {'dp': ((at['z'] * side + at['y']) * side + at['x']) * 2 + k}

    partner = {'dp': chip * 2 + other}
    hops = lambda d: min(d, side - d)
    axis_shifts = sorted(range(1, side), key=hops, reverse=True)
    plane_shifts = sorted(
        [(i, j) for i in range(side) for j in range(side) if i or j],
        key=lambda s: hops(s[0]) + hops(s[1]), reverse=True)

    def wq_copy(layer, i):
        cols = pl.ds(pl.multiple_of(core * qw + i * q_chunk, 128), q_chunk)
        return pltpu.make_async_copy(wq_hbm.at[layer, :, cols], wq.at[i], wq_sem.at[i])

    def wo_copy(layer, i):
        depth = pl.ds(pl.multiple_of(core * kdim, 128), kdim)
        cols = pl.ds(pl.multiple_of(i * o_chunk, 128), o_chunk)
        return pltpu.make_async_copy(wo_hbm.at[layer, depth, cols], wo.at[i], wo_sem.at[i])

    def cache_copy(layer, b):
        return pltpu.make_async_copy(cache_hbm.at[layer, b], cbuf.at[layer, b], c_sem.at[layer, b])

    ffn_pairs = ((wg_hbm, wg), (wu_hbm, wu), (wd_hbm, wd))

    def ffn_copies(layer):
        return [
            pltpu.make_async_copy(src.at[layer], dst.at[layer, core], f_sem.at[layer, i])
            for i, (src, dst) in enumerate(ffn_pairs)]

    inputs = [
        pltpu.make_async_copy(src, dst, in_sem.at[i])
        for i, (src, dst) in enumerate(((x_hbm, xin), (len_hbm, lens), (ag_hbm, ag), (fg_hbm, fg)))]
    for copy in inputs:
        copy.start()
    for i in range(n_q):
        wq_copy(0, i).start()
    for b in range(2):
        cache_copy(0, b).start()
    for i in range(n_o):
        wo_copy(0, i).start()

    barrier = pltpu.get_barrier_semaphore()
    peers = [partner] + [
        device(**shift) for shift in
        [{a: d} for a in 'zyx' for d in range(1, side)]
        + [{a: d, b: e} for a, b in ('zy', 'zx', 'yx') for d in range(1, side) for e in range(1, side)]]
    for peer in peers:
        pl.semaphore_signal(barrier, inc=1, device_id=peer, device_id_type=MESH)
    pl.semaphore_wait(barrier, len(peers))

    pending = []

    def remote(layer, index, src, dst, peer):
        return pltpu.make_async_remote_copy(
            src_ref=src, dst_ref=dst, send_sem=ssem.at[layer, index], recv_sem=rsem.at[layer, index],
            device_id=peer, device_id_type=MESH)

    def send(layer, index, src, dst, peer):
        copy = remote(layer, index, src, dst, peer)
        copy.start()
        pending.append(copy)

    def recv(layer, index, dst, peer):
        remote(layer, index, dst, dst, peer).wait_recv()

    def send_weights(layer):
        for b in range(2):
            send(layer, 2 + b, cache_hbm.at[layer, b], cbuf.at[layer, 2 + b], partner)
        for i, (src, dst) in enumerate(ffn_pairs):
            send(layer, 4 + i, src.at[layer], dst.at[layer, core], partner)

    for copy in inputs:
        copy.wait()
    xsend[0] = xin[...].astype(F32)
    send(0, 0, xsend.at[0], xrecv.at[0], partner)
    for b in range(2):
        lbuf[0, b:b + 1, :] = jnp.full((1, 128), lens[b], jnp.int32).astype(F32)
    send(0, 7, lbuf.at[0], lbuf.at[1], partner)
    send_weights(0)
    for layer in range(layers):
        for copy in ffn_copies(layer):
            copy.start()
    lhs[4:8, :] = jnp.zeros((4, kdim), F32)

    def rms(v, gain):
        mean_sq = jnp.mean(v * v, axis=-1, keepdims=True)
        return v * lax.rsqrt(mean_sq + NORM_EPS) * gain

    def attention(layer, x2):
        recv(layer, 0, xrecv.at[layer], partner)
        if layer == 0:
            recv(0, 7, lbuf.at[1], partner)
        x4 = jnp.concatenate([x2, xrecv[layer]], axis=0)
        normed = rms(x4, ag[layer:layer + 1, :])
        h8 = jnp.concatenate([normed, normed], axis=0).astype(BF16)

        def q_step(i, carry):
            wq_copy(layer, i).wait()
            qrow[:, pl.ds(pl.multiple_of(i * q_chunk, 128), q_chunk)] = dot(h8, wq[i])
            return carry

        lax.fori_loop(0, n_q, q_step, 0)
        if layer + 1 < layers:
            for i in range(n_q):
                wq_copy(layer + 1, i).start()
            for b in range(2):
                cache_copy(layer + 1, b).start()
            send_weights(layer + 1)
        pair = 2 * kv
        for j in range(heads_half // 2):
            block = qrow[:, j * pair:(j + 1) * pair]
            odd = pltpu.roll(block[:, latent:latent + 640], 640 - 64, 1)
            for parity, q8 in ((0, block[:, :640]), (1, odd)):
                h = 2 * j + parity
                for b in range(4):
                    qbuf[b, h:h + 1, :] = q8[b:b + 1, :]
        positions = lax.broadcasted_iota(jnp.int32, (heads_half, seq), 1).astype(F32)
        for b in range(2):
            cache_copy(layer, b).wait()
        for b in range(2):
            recv(layer, 2 + b, cbuf.at[layer, 2 + b], partner)
        for b in range(4):
            q = qbuf[b][:, :kv].astype(BF16)
            s = dot(q, cbuf[layer, b]) * scale
            length = lbuf[b // 2, b % 2:b % 2 + 1, 0:1]
            s = jnp.where(positions < length, s, -jnp.inf)
            e = jnp.exp(s - jnp.max(s, axis=-1, keepdims=True))
            p = (e / jnp.sum(e, axis=-1, keepdims=True)).astype(BF16)
            o = dot_nt(p, cbuf[layer, b, :latent, :])
            for h in range(heads_half):
                lhs[b:b + 1, h * latent:(h + 1) * latent] = o[h:h + 1, :]
        lhs_b = lhs[...].astype(BF16)

        def o_step(i, carry):
            wo_copy(layer, i).wait()
            y = dot(lhs_b, wo[i])
            cols = pl.ds(pl.multiple_of(i * o_chunk, 128), o_chunk)
            ysend[layer, 0, :, cols] = y[0:2]
            ysend[layer, 1, :, cols] = y[2:4]
            return carry

        lax.fori_loop(0, n_o, o_step, 0)
        send(layer, 1, ysend.at[layer, 1], yrecv.at[layer], partner)
        if layer + 1 < layers:
            for i in range(n_o):
                wo_copy(layer + 1, i).start()
        recv(layer, 1, yrecv.at[layer], partner)
        return (x2 + (ysend[layer, 0] + yrecv[layer])).astype(BF16).astype(F32)

    def slot(c):
        _, a, b = COLOURS[c]
        return coord[a] * side + coord[b]

    def plane_wait(buf, layer, send_sem, recv_sem, c, sent):
        part = buf.at[layer, pl.ds(0, plane - 1)]
        copy = pltpu.make_async_remote_copy(
            src_ref=part, dst_ref=part, send_sem=send_sem.at[layer, c], recv_sem=recv_sem.at[layer, c],
            device_id=partner, device_id_type=MESH)
        return copy.wait_send() if sent else copy.wait_recv()

    def natural_of(index):
        log = side.bit_length() - 1
        r = index & 1
        at = {'x': (index >> 1) & (side - 1), 'y': (index >> (1 + log)) & (side - 1), 'z': index >> (1 + 2 * log)}
        return [
            (((at[o] << (2 * log)) | (at[a] << log) | at[b]) << 1) | r for o, a, b in COLOURS]

    def ffn(layer, x2):
        g2 = rms(x2, fg[layer:layer + 1, :]).astype(BF16)
        for c, (base, width) in enumerate(columns):
            _, a, b = COLOURS[c]
            p1[c][layer, slot(c)] = g2[:, base:base + width]
            for i, j in plane_shifts:
                block = p1[c].at[layer, slot(c)]
                pltpu.make_async_remote_copy(
                    src_ref=block, dst_ref=block, send_sem=agp_s.at[layer, c], recv_sem=agp_r.at[layer, c],
                    device_id=device(**{a: i, b: j}), device_id_type=MESH).start()
        for c, (base, width) in enumerate(columns):
            axis = COLOURS[c][0]
            plane_wait(p1[c], layer, agp_s, agp_r, c, False)
            for i in range(plane):
                asm[2 * i:2 * i + 2, base:base + width] = p1[c][layer, i].astype(F32)
            g_buf[c][layer, coord[axis]] = asm[:, base:base + width].astype(BF16)
            own = g_buf[c].at[layer, coord[axis]]
            for d in axis_shifts:
                send(layer, 8 + 3 * c + d - 1, own, own, device(**{axis: d}))
        for copy in ffn_copies(layer):
            copy.wait()
        for i, (_, dst) in enumerate(ffn_pairs):
            recv(layer, 4 + i, dst.at[layer, other], partner)

        across = lax.broadcasted_iota(jnp.int32, (rows, rows), 1)
        down = lax.broadcasted_iota(jnp.int32, (rows, rows), 0)
        parts = []
        for c, (base, width) in enumerate(columns):
            axis = COLOURS[c][0]
            for d in axis_shifts:
                recv(layer, 8 + 3 * c + d - 1, g_buf[c].at[layer, step(coord[axis], side - d)], device(**{axis: d}))
            part = g_buf[c][layer].reshape(rows, width)
            if c:
                pick = (natural_of(down)[c] == across).astype(F32).astype(BF16)
                part = dot(pick, part).astype(BF16)
            parts.append(part)
        g = jnp.concatenate(parts, axis=1)
        hidden = []
        for k in range(2):
            gate = dot_nt(g, wg[layer, k])
            up = dot_nt(g, wu[layer, k])
            hidden.append((jax.nn.silu(gate) * up).astype(BF16))

        for c, (base, width) in enumerate(columns):
            axis = COLOURS[c][0]
            total = None
            for k in range(2):
                a = hidden[k]
                if c:
                    pick = (natural_of(across)[c] == down).astype(F32).astype(BF16)
                    a = dot(pick, a).astype(BF16)
                term = dot(a, wd[layer, k, :, base:base + width])
                total = term if total is None else total + term
            s_buf[c][layer] = total.reshape(side, 2 * plane, width)
            for d in axis_shifts:
                send(layer, 17 + 3 * c + d - 1, s_buf[c].at[layer, step(coord[axis], d)], r1[c].at[layer, d - 1],
                     device(**{axis: d}))
        for c, (base, width) in enumerate(columns):
            axis, a, b = COLOURS[c]
            total = s_buf[c][layer, coord[axis]]
            for d in axis_shifts:
                recv(layer, 17 + 3 * c + d - 1, r1[c].at[layer, d - 1], device(**{axis: d}))
                total = total + r1[c][layer, d - 1]
            for i in range(plane):
                u_buf[c][layer, i] = total[2 * i:2 * i + 2]
            for i, j in plane_shifts:
                target = step(coord[a], i) * side + step(coord[b], j)
                pltpu.make_async_remote_copy(
                    src_ref=u_buf[c].at[layer, target], dst_ref=r2[c].at[layer, slot(c)],
                    send_sem=rsp_s.at[layer, c], recv_sem=rsp_r.at[layer, c],
                    device_id=device(**{a: i, b: j}), device_id_type=MESH).start()
        sums = []
        for c in range(3):
            r2[c][layer, slot(c)] = u_buf[c][layer, slot(c)]
            plane_wait(r2[c], layer, rsp_s, rsp_r, c, False)
            total = r2[c][layer, 0]
            for i in range(1, plane):
                total = total + r2[c][layer, i]
            sums.append(total)
        return (x2 + jnp.concatenate(sums, axis=1)).astype(BF16).astype(F32)

    x2 = xsend[0]
    for layer in range(layers):
        x2 = attention(layer, x2)
        x2 = ffn(layer, x2)
        if layer + 1 < layers:
            xsend[layer + 1] = x2
            send(layer + 1, 0, xsend.at[layer + 1], xrecv.at[layer + 1], partner)
    out_ref[...] = x2
    for copy in pending:
        copy.wait_send()
    for layer in range(layers):
        for c in range(3):
            plane_wait(p1[c], layer, agp_s, agp_r, c, True)
            plane_wait(u_buf[c], layer, rsp_s, rsp_r, c, True)


def solution(mesh):
    devices = mesh.shape['dp']
    side = round((devices // 2) ** (1 / 3))

    def local_step(x, lengths, cache, attn_gain, ffn_gain, w_query, w_attn_out, w_up, w_gate, w_down):
        layers, _, seq, kv = cache.shape
        d_model = x.shape[1]
        heads = w_query.shape[2] // kv
        latent = w_attn_out.shape[1] // heads
        hid = w_up.shape[2]
        hh = heads // 2
        q_chunk, o_chunk = 512, 256
        n_q, n_o = hh * kv // q_chunk, d_model // o_chunk
        plane = side * side
        widths = [w for _, w in colour_columns(d_model)]
        cfg = (side, layers, heads, kv, latent, seq, d_model, q_chunk, o_chunk)
        hbm = pl.BlockSpec(memory_space=pl.ANY)
        scratch = [
            pltpu.VMEM((n_q, d_model, q_chunk), BF16),
            pltpu.VMEM((n_o, hh * latent, o_chunk), BF16),
            pltpu.VMEM((layers, 4, kv, seq), BF16),
            pltpu.VMEM((layers, 2, hid, d_model), BF16),
            pltpu.VMEM((layers, 2, hid, d_model), BF16),
            pltpu.VMEM((layers, 2, hid, d_model), BF16),
            pltpu.VMEM((2, d_model), BF16),
            pltpu.SMEM((2,), jnp.int32),
            pltpu.VMEM((layers, d_model), F32),
            pltpu.VMEM((layers, d_model), F32),
            pltpu.VMEM((2, 2, 128), F32),
            pltpu.VMEM((layers, 2, d_model), F32),
            pltpu.VMEM((layers, 2, d_model), F32),
            pltpu.VMEM((8, hh * kv), F32),
            pltpu.VMEM((4, hh, 640), F32),
            pltpu.VMEM((8, hh * latent), F32),
            pltpu.VMEM((layers, 2, 2, d_model), F32),
            pltpu.VMEM((layers, 2, d_model), F32),
            pltpu.VMEM((2 * plane, d_model), F32),
            *[pltpu.VMEM((layers, plane, 2, w), BF16) for w in widths],
            *[pltpu.VMEM((layers, side, 2 * plane, w), BF16) for w in widths],
            *[pltpu.VMEM((layers, side, 2 * plane, w), F32) for w in widths],
            *[pltpu.VMEM((layers, side - 1, 2 * plane, w), F32) for w in widths],
            *[pltpu.VMEM((layers, plane, 2, w), F32) for w in widths],
            *[pltpu.VMEM((layers, plane, 2, w), F32) for w in widths],
            pltpu.SemaphoreType.DMA((n_q,)),
            pltpu.SemaphoreType.DMA((n_o,)),
            pltpu.SemaphoreType.DMA((layers, 2)),
            pltpu.SemaphoreType.DMA((layers, 3)),
            pltpu.SemaphoreType.DMA((4,)),
            pltpu.SemaphoreType.DMA((layers, 26)),
            pltpu.SemaphoreType.DMA((layers, 26)),
            *[pltpu.SemaphoreType.DMA((layers, 3)) for _ in range(4)],
        ]
        out = pl.pallas_call(
            functools.partial(kernel, cfg),
            out_shape=jax.ShapeDtypeStruct(x.shape, F32),
            in_specs=[hbm] * 10,
            out_specs=pl.BlockSpec(memory_space=pltpu.VMEM),
            scratch_shapes=scratch,
            compiler_params=pltpu.CompilerParams(
                collective_id=0, has_side_effects=True, vmem_limit_bytes=66_500_000),
            name='mla_decode',
        )(x, lengths, attn_gain, ffn_gain, jnp.swapaxes(cache, 2, 3), w_query, w_attn_out,
          jnp.swapaxes(w_up, 1, 2), jnp.swapaxes(w_gate, 1, 2), w_down)
        return out.astype(BF16)

    rows = ('replica', 'dp')
    return jax.shard_map(
        local_step,
        mesh=mesh,
        in_specs=(P(rows, None), P(rows), P(None, rows, None, None), P(), P(), P(), P(),
                  P(None, None, 'dp'), P(None, None, 'dp'), P(None, 'dp', None)),
        out_specs=P(rows, None),
        check_vma=False,
    )
```

```python
import functools

import jax
import jax.numpy as jnp
from jax import lax
from jax.experimental import pallas as pl
from jax.experimental.pallas import tpu as pltpu
from jax.sharding import PartitionSpec as P

NORM_EPS = 1e-6
MESH = pl.DeviceIdType.MESH
F32 = jnp.float32
BF16 = jnp.bfloat16
COLOURS = (('z', 'y', 'x'), ('x', 'z', 'y'), ('y', 'z', 'x'))


def dot(a, b):
    return jnp.dot(a, b, preferred_element_type=F32)


def dot_nt(a, b):
    return lax.dot_general(a, b, (((1,), (1,)), ((), ())), preferred_element_type=F32)


def colour_columns(d_model):
    tiles = d_model // 128
    widths = [128 * ((tiles + 2 - c) // 3) for c in range(3)]
    return [(sum(widths[:c]), widths[c]) for c in range(3)]


def kernel(
    cfg,
    x_hbm, len_hbm, ag_hbm, fg_hbm, cache_hbm, wq_hbm, wo_hbm, wu_hbm, wg_hbm, wd_hbm,
    out_ref,
    wq, wo, cbuf, wu, wg, wd,
    xin, lens, ag, fg, lbuf, xsend, xrecv, qrow, qbuf, lhs, ysend, yrecv, asm,
    p1a, p1b, p1c, g_a, g_b, g_c, s_a, s_b, s_c, r1a, r1b, r1c, u_a, u_b, u_c, r2a, r2b, r2c,
    wq_sem, wo_sem, c_sem, f_sem, in_sem, ssem, rsem, agp_s, agp_r, rsp_s, rsp_r,
):
    side, layers, heads, kv, latent, seq, d_model, q_chunk, o_chunk = cfg
    heads_half = heads // 2
    qw = heads_half * kv
    n_q = qw // q_chunk
    n_o = d_model // o_chunk
    kdim = heads_half * latent
    plane = side * side
    rows = 2 * side ** 3
    scale = (3 * (kv - latent)) ** -0.5
    columns = colour_columns(d_model)
    p1, g_buf, s_buf = (p1a, p1b, p1c), (g_a, g_b, g_c), (s_a, s_b, s_c)
    r1, u_buf, r2 = (r1a, r1b, r1c), (u_a, u_b, u_c), (r2a, r2b, r2c)

    me = lax.axis_index('dp')
    core = lax.rem(me, 2)
    chip = lax.div(me, 2)
    coord = {'x': lax.rem(chip, side), 'y': lax.rem(lax.div(chip, side), side), 'z': lax.div(chip, plane)}
    other = 1 - core

    def step(c, d):
        return lax.rem(c + d, side)

    def device(k=core, **shift):
        at = {a: step(coord[a], shift.get(a, 0)) for a in 'zyx'}
        return {'dp': ((at['z'] * side + at['y']) * side + at['x']) * 2 + k}

    partner = {'dp': chip * 2 + other}
    hops = lambda d: min(d, side - d)
    axis_shifts = sorted(range(1, side), key=hops, reverse=True)
    plane_shifts = sorted(
        [(i, j) for i in range(side) for j in range(side) if i or j],
        key=lambda s: hops(s[0]) + hops(s[1]), reverse=True)

    def wq_copy(layer, i):
        cols = pl.ds(pl.multiple_of(core * qw + i * q_chunk, 128), q_chunk)
        return pltpu.make_async_copy(wq_hbm.at[layer, :, cols], wq.at[i], wq_sem.at[i])

    def wo_copy(layer, i):
        depth = pl.ds(pl.multiple_of(core * kdim, 128), kdim)
        cols = pl.ds(pl.multiple_of(i * o_chunk, 128), o_chunk)
        return pltpu.make_async_copy(wo_hbm.at[layer, depth, cols], wo.at[i], wo_sem.at[i])

    def cache_copy(layer, b):
        return pltpu.make_async_copy(cache_hbm.at[layer, b], cbuf.at[layer, b], c_sem.at[layer, b])

    ffn_pairs = ((wg_hbm, wg), (wu_hbm, wu), (wd_hbm, wd))

    def ffn_copies(layer):
        return [
            pltpu.make_async_copy(src.at[layer], dst.at[layer, core], f_sem.at[layer, i])
            for i, (src, dst) in enumerate(ffn_pairs)]

    inputs = [
        pltpu.make_async_copy(src, dst, in_sem.at[i])
        for i, (src, dst) in enumerate(((x_hbm, xin), (len_hbm, lens), (ag_hbm, ag), (fg_hbm, fg)))]
    for copy in inputs:
        copy.start()
    for b in range(2):
        cache_copy(0, b).start()
    for i in range(n_q):
        wq_copy(0, i).start()
    for copy in ffn_copies(0):
        copy.start()
    for i in range(n_o):
        wo_copy(0, i).start()

    barrier = pltpu.get_barrier_semaphore()
    peers = [partner] + [
        device(**shift) for shift in
        [{a: d} for a in 'zyx' for d in range(1, side)]
        + [{a: d, b: e} for a, b in ('zy', 'zx', 'yx') for d in range(1, side) for e in range(1, side)]]
    for peer in peers:
        pl.semaphore_signal(barrier, inc=1, device_id=peer, device_id_type=MESH)
    pl.semaphore_wait(barrier, len(peers))

    pending = []

    def remote(layer, index, src, dst, peer):
        return pltpu.make_async_remote_copy(
            src_ref=src, dst_ref=dst, send_sem=ssem.at[layer, index], recv_sem=rsem.at[layer, index],
            device_id=peer, device_id_type=MESH)

    def send(layer, index, src, dst, peer):
        copy = remote(layer, index, src, dst, peer)
        copy.start()
        pending.append(copy)

    def recv(layer, index, dst, peer):
        remote(layer, index, dst, dst, peer).wait_recv()

    def send_cache(layer, src):
        for b in range(2):
            send(layer, 2 + b, src.at[layer, b], cbuf.at[layer, 2 + b], partner)

    def send_ffn(layer, local):
        for i, (src, dst) in enumerate(ffn_pairs):
            src = dst.at[layer, core] if local else src.at[layer]
            send(layer, 4 + i, src, dst.at[layer, core], partner)

    for copy in inputs:
        copy.wait()
    xsend[0] = xin[...].astype(F32)
    send(0, 0, xsend.at[0], xrecv.at[0], partner)
    for b in range(2):
        lbuf[0, b:b + 1, :] = jnp.full((1, 128), lens[b], jnp.int32).astype(F32)
    send(0, 7, lbuf.at[0], lbuf.at[1], partner)
    for b in range(2):
        cache_copy(0, b).wait()
    send_cache(0, cbuf)
    lhs[4:8, :] = jnp.zeros((4, kdim), F32)

    def rms(v, gain):
        mean_sq = jnp.mean(v * v, axis=-1, keepdims=True)
        return v * lax.rsqrt(mean_sq + NORM_EPS) * gain

    def attention(layer, x2):
        recv(layer, 0, xrecv.at[layer], partner)
        if layer == 0:
            recv(0, 7, lbuf.at[1], partner)
        x4 = jnp.concatenate([x2, xrecv[layer]], axis=0)
        normed = rms(x4, ag[layer:layer + 1, :])
        h8 = jnp.concatenate([normed, normed], axis=0).astype(BF16)

        def q_step(i, carry):
            wq_copy(layer, i).wait()
            qrow[:, pl.ds(pl.multiple_of(i * q_chunk, 128), q_chunk)] = dot(h8, wq[i])
            return carry

        lax.fori_loop(0, n_q, q_step, 0)
        for copy in ffn_copies(layer):
            copy.wait()
        if layer == 0:
            send_ffn(layer, True)
        pair = 2 * kv
        for j in range(heads_half // 2):
            block = qrow[:, j * pair:(j + 1) * pair]
            odd = pltpu.roll(block[:, latent:latent + 640], 640 - 64, 1)
            for parity, q8 in ((0, block[:, :640]), (1, odd)):
                h = 2 * j + parity
                for b in range(4):
                    qbuf[b, h:h + 1, :] = q8[b:b + 1, :]
        positions = lax.broadcasted_iota(jnp.int32, (heads_half, seq), 1).astype(F32)
        if layer:
            for b in range(2):
                cache_copy(layer, b).wait()
        for b in range(2):
            recv(layer, 2 + b, cbuf.at[layer, 2 + b], partner)
        for b in range(4):
            q = qbuf[b][:, :kv].astype(BF16)
            s = dot(q, cbuf[layer, b]) * scale
            length = lbuf[b // 2, b % 2:b % 2 + 1, 0:1]
            s = jnp.where(positions < length, s, -jnp.inf)
            e = jnp.exp(s - jnp.max(s, axis=-1, keepdims=True))
            p = (e / jnp.sum(e, axis=-1, keepdims=True)).astype(BF16)
            o = dot_nt(p, cbuf[layer, b, :latent, :])
            for h in range(heads_half):
                lhs[b:b + 1, h * latent:(h + 1) * latent] = o[h:h + 1, :]
        lhs_b = lhs[...].astype(BF16)

        def o_step(i, carry):
            wo_copy(layer, i).wait()
            y = dot(lhs_b, wo[i])
            cols = pl.ds(pl.multiple_of(i * o_chunk, 128), o_chunk)
            ysend[layer, 0, :, cols] = y[0:2]
            ysend[layer, 1, :, cols] = y[2:4]
            return carry

        lax.fori_loop(0, n_o, o_step, 0)
        send(layer, 1, ysend.at[layer, 1], yrecv.at[layer], partner)
        if layer + 1 < layers:
            for b in range(2):
                cache_copy(layer + 1, b).start()
            for copy in ffn_copies(layer + 1):
                copy.start()
            for i in range(n_q):
                wq_copy(layer + 1, i).start()
            for i in range(n_o):
                wo_copy(layer + 1, i).start()
        recv(layer, 1, yrecv.at[layer], partner)
        return (x2 + (ysend[layer, 0] + yrecv[layer])).astype(BF16).astype(F32)

    def slot(c):
        _, a, b = COLOURS[c]
        return coord[a] * side + coord[b]

    def plane_wait(buf, layer, send_sem, recv_sem, c, sent):
        part = buf.at[layer, pl.ds(0, plane - 1)]
        copy = pltpu.make_async_remote_copy(
            src_ref=part, dst_ref=part, send_sem=send_sem.at[layer, c], recv_sem=recv_sem.at[layer, c],
            device_id=partner, device_id_type=MESH)
        return copy.wait_send() if sent else copy.wait_recv()

    def natural_of(index):
        log = side.bit_length() - 1
        r = index & 1
        at = {'x': (index >> 1) & (side - 1), 'y': (index >> (1 + log)) & (side - 1), 'z': index >> (1 + 2 * log)}
        return [
            (((at[o] << (2 * log)) | (at[a] << log) | at[b]) << 1) | r for o, a, b in COLOURS]

    def ffn(layer, x2):
        g2 = rms(x2, fg[layer:layer + 1, :]).astype(BF16)
        for c, (base, width) in enumerate(columns):
            _, a, b = COLOURS[c]
            p1[c][layer, slot(c)] = g2[:, base:base + width]
            for i, j in plane_shifts:
                block = p1[c].at[layer, slot(c)]
                pltpu.make_async_remote_copy(
                    src_ref=block, dst_ref=block, send_sem=agp_s.at[layer, c], recv_sem=agp_r.at[layer, c],
                    device_id=device(**{a: i, b: j}), device_id_type=MESH).start()
        if layer + 1 < layers:
            send_cache(layer + 1, cache_hbm)
            send_ffn(layer + 1, False)
        for c, (base, width) in enumerate(columns):
            axis = COLOURS[c][0]
            plane_wait(p1[c], layer, agp_s, agp_r, c, False)
            for i in range(plane):
                asm[2 * i:2 * i + 2, base:base + width] = p1[c][layer, i].astype(F32)
            g_buf[c][layer, coord[axis]] = asm[:, base:base + width].astype(BF16)
            own = g_buf[c].at[layer, coord[axis]]
            for d in axis_shifts:
                send(layer, 8 + 3 * c + d - 1, own, own, device(**{axis: d}))
        for i, (_, dst) in enumerate(ffn_pairs):
            recv(layer, 4 + i, dst.at[layer, other], partner)

        across = lax.broadcasted_iota(jnp.int32, (rows, rows), 1)
        down = lax.broadcasted_iota(jnp.int32, (rows, rows), 0)
        parts = []
        for c, (base, width) in enumerate(columns):
            axis = COLOURS[c][0]
            for d in axis_shifts:
                recv(layer, 8 + 3 * c + d - 1, g_buf[c].at[layer, step(coord[axis], side - d)], device(**{axis: d}))
            part = g_buf[c][layer].reshape(rows, width)
            if c:
                pick = (natural_of(down)[c] == across).astype(F32).astype(BF16)
                part = dot(pick, part).astype(BF16)
            parts.append(part)
        g = jnp.concatenate(parts, axis=1)
        hidden = []
        for k in range(2):
            gate = dot_nt(g, wg[layer, k])
            up = dot_nt(g, wu[layer, k])
            hidden.append((jax.nn.silu(gate) * up).astype(BF16))

        for c, (base, width) in enumerate(columns):
            axis = COLOURS[c][0]
            total = None
            for k in range(2):
                a = hidden[k]
                if c:
                    pick = (natural_of(across)[c] == down).astype(F32).astype(BF16)
                    a = dot(pick, a).astype(BF16)
                term = dot(a, wd[layer, k, :, base:base + width])
                total = term if total is None else total + term
            s_buf[c][layer] = total.reshape(side, 2 * plane, width)
            for d in axis_shifts:
                send(layer, 17 + 3 * c + d - 1, s_buf[c].at[layer, step(coord[axis], d)], r1[c].at[layer, d - 1],
                     device(**{axis: d}))
        for c, (base, width) in enumerate(columns):
            axis, a, b = COLOURS[c]
            total = s_buf[c][layer, coord[axis]]
            for d in axis_shifts:
                recv(layer, 17 + 3 * c + d - 1, r1[c].at[layer, d - 1], device(**{axis: d}))
                total = total + r1[c][layer, d - 1]
            for i in range(plane):
                u_buf[c][layer, i] = total[2 * i:2 * i + 2]
            for i, j in plane_shifts:
                target = step(coord[a], i) * side + step(coord[b], j)
                pltpu.make_async_remote_copy(
                    src_ref=u_buf[c].at[layer, target], dst_ref=r2[c].at[layer, slot(c)],
                    send_sem=rsp_s.at[layer, c], recv_sem=rsp_r.at[layer, c],
                    device_id=device(**{a: i, b: j}), device_id_type=MESH).start()
        sums = []
        for c in range(3):
            r2[c][layer, slot(c)] = u_buf[c][layer, slot(c)]
            plane_wait(r2[c], layer, rsp_s, rsp_r, c, False)
            total = r2[c][layer, 0]
            for i in range(1, plane):
                total = total + r2[c][layer, i]
            sums.append(total)
        return (x2 + jnp.concatenate(sums, axis=1)).astype(BF16).astype(F32)

    x2 = xsend[0]
    for layer in range(layers):
        x2 = attention(layer, x2)
        x2 = ffn(layer, x2)
        if layer + 1 < layers:
            xsend[layer + 1] = x2
            send(layer + 1, 0, xsend.at[layer + 1], xrecv.at[layer + 1], partner)
    out_ref[...] = x2
    for copy in pending:
        copy.wait_send()
    for layer in range(layers):
        for c in range(3):
            plane_wait(p1[c], layer, agp_s, agp_r, c, True)
            plane_wait(u_buf[c], layer, rsp_s, rsp_r, c, True)


def solution(mesh):
    devices = mesh.shape['dp']
    side = round((devices // 2) ** (1 / 3))

    def local_step(x, lengths, cache, attn_gain, ffn_gain, w_query, w_attn_out, w_up, w_gate, w_down):
        layers, _, seq, kv = cache.shape
        d_model = x.shape[1]
        heads = w_query.shape[2] // kv
        latent = w_attn_out.shape[1] // heads
        hid = w_up.shape[2]
        hh = heads // 2
        q_chunk, o_chunk = 512, 256
        n_q, n_o = hh * kv // q_chunk, d_model // o_chunk
        plane = side * side
        widths = [w for _, w in colour_columns(d_model)]
        cfg = (side, layers, heads, kv, latent, seq, d_model, q_chunk, o_chunk)
        hbm = pl.BlockSpec(memory_space=pl.ANY)
        scratch = [
            pltpu.VMEM((n_q, d_model, q_chunk), BF16),
            pltpu.VMEM((n_o, hh * latent, o_chunk), BF16),
            pltpu.VMEM((layers, 4, kv, seq), BF16),
            pltpu.VMEM((layers, 2, hid, d_model), BF16),
            pltpu.VMEM((layers, 2, hid, d_model), BF16),
            pltpu.VMEM((layers, 2, hid, d_model), BF16),
            pltpu.VMEM((2, d_model), BF16),
            pltpu.SMEM((2,), jnp.int32),
            pltpu.VMEM((layers, d_model), F32),
            pltpu.VMEM((layers, d_model), F32),
            pltpu.VMEM((2, 2, 128), F32),
            pltpu.VMEM((layers, 2, d_model), F32),
            pltpu.VMEM((layers, 2, d_model), F32),
            pltpu.VMEM((8, hh * kv), F32),
            pltpu.VMEM((4, hh, 640), F32),
            pltpu.VMEM((8, hh * latent), F32),
            pltpu.VMEM((layers, 2, 2, d_model), F32),
            pltpu.VMEM((layers, 2, d_model), F32),
            pltpu.VMEM((2 * plane, d_model), F32),
            *[pltpu.VMEM((layers, plane, 2, w), BF16) for w in widths],
            *[pltpu.VMEM((layers, side, 2 * plane, w), BF16) for w in widths],
            *[pltpu.VMEM((layers, side, 2 * plane, w), F32) for w in widths],
            *[pltpu.VMEM((layers, side - 1, 2 * plane, w), F32) for w in widths],
            *[pltpu.VMEM((layers, plane, 2, w), F32) for w in widths],
            *[pltpu.VMEM((layers, plane, 2, w), F32) for w in widths],
            pltpu.SemaphoreType.DMA((n_q,)),
            pltpu.SemaphoreType.DMA((n_o,)),
            pltpu.SemaphoreType.DMA((layers, 2)),
            pltpu.SemaphoreType.DMA((layers, 3)),
            pltpu.SemaphoreType.DMA((4,)),
            pltpu.SemaphoreType.DMA((layers, 26)),
            pltpu.SemaphoreType.DMA((layers, 26)),
            *[pltpu.SemaphoreType.DMA((layers, 3)) for _ in range(4)],
        ]
        out = pl.pallas_call(
            functools.partial(kernel, cfg),
            out_shape=pltpu.VMEM(x.shape, F32),
            in_specs=[hbm] * 10,
            out_specs=pl.BlockSpec(memory_space=pltpu.VMEM),
            scratch_shapes=scratch,
            compiler_params=pltpu.CompilerParams(
                collective_id=0, has_side_effects=True, vmem_limit_bytes=66_500_000),
            name='mla_decode',
        )(x, lengths, attn_gain, ffn_gain, jnp.swapaxes(cache, 2, 3), w_query, w_attn_out,
          jnp.swapaxes(w_up, 1, 2), jnp.swapaxes(w_gate, 1, 2), w_down)
        return out.astype(BF16)

    rows = ('replica', 'dp')
    return jax.shard_map(
        local_step,
        mesh=mesh,
        in_specs=(P(rows, None), P(rows), P(None, rows, None, None), P(), P(), P(), P(),
                  P(None, None, 'dp'), P(None, None, 'dp'), P(None, 'dp', None)),
        out_specs=P(rows, None),
        check_vma=False,
    )
```

```python
import functools

import jax
import jax.numpy as jnp
from jax import lax
from jax.experimental import pallas as pl
from jax.experimental.pallas import tpu as pltpu
from jax.sharding import PartitionSpec as P

NORM_EPS = 1e-6
MESH = pl.DeviceIdType.MESH
F32 = jnp.float32
BF16 = jnp.bfloat16
COLOURS = (('z', 'y', 'x'), ('x', 'z', 'y'), ('y', 'z', 'x'))


def dot(a, b):
    return jnp.dot(a, b, preferred_element_type=F32)


def dot_nt(a, b):
    return lax.dot_general(a, b, (((1,), (1,)), ((), ())), preferred_element_type=F32)


def colour_columns(d_model):
    tiles = d_model // 128
    widths = [128 * ((tiles + 2 - c) // 3) for c in range(3)]
    return [(sum(widths[:c]), widths[c]) for c in range(3)]


def kernel(
    cfg,
    x_hbm, len_hbm, ag_hbm, fg_hbm, cache_hbm, wq_hbm, wo_hbm, wu_hbm, wg_hbm, wd_hbm,
    out_ref,
    wq, wo, cbuf, wgu, wd,
    xin, lens, ag, fg, lbuf, xall, qrow, qbuf, lhs, ypart, yrecv, asm, hid, pick,
    gin, s_a, s_b, s_c, r1a, r1b, r1c, u_a, u_b, u_c, r2a, r2b, r2c,
    wq_sem, wo_sem, c_sem, f_sem, in_sem, ssem, rsem, ag_s, ag_r, rsp_s, rsp_r,
):
    side, layers, heads, kv, latent, seq, d_model, hid_dim, q_chunk, o_chunk = cfg
    heads_half = heads // 2
    qw = heads_half * kv
    n_q = qw // q_chunk
    n_o = d_model // o_chunk
    kdim = heads_half * latent
    plane = side * side
    group = 2 * plane
    rows = group * side
    scale = (3 * (kv - latent)) ** -0.5
    columns = colour_columns(d_model)
    s_buf, r1, u_buf, r2 = (s_a, s_b, s_c), (r1a, r1b, r1c), (u_a, u_b, u_c), (r2a, r2b, r2c)

    me = lax.axis_index('dp')
    core = lax.rem(me, 2)
    chip = lax.div(me, 2)
    coord = {'x': lax.rem(chip, side), 'y': lax.rem(lax.div(chip, side), side), 'z': lax.div(chip, plane)}
    other = 1 - core

    def step(c, d):
        return lax.rem(c + d, side)

    def device(**shift):
        at = {a: step(coord[a], shift.get(a, 0)) for a in 'zyx'}
        return {'dp': ((at['z'] * side + at['y']) * side + at['x']) * 2 + core}

    def hops(*shift):
        return sum(min(d, side - d) for d in shift)

    partner = {'dp': chip * 2 + other}
    axis_shifts = sorted(range(1, side), key=hops, reverse=True)
    plane_shifts = sorted(
        [(i, j) for i in range(side) for j in range(side) if i or j], key=lambda s: hops(*s), reverse=True)
    cube_shifts = sorted(
        [(i, j, k) for i in range(side) for j in range(side) for k in range(side) if i or j or k],
        key=lambda s: hops(*s), reverse=True)

    def wq_copy(layer, i):
        cols = pl.ds(pl.multiple_of(core * qw + i * q_chunk, 128), q_chunk)
        return pltpu.make_async_copy(wq_hbm.at[layer, :, cols], wq.at[i], wq_sem.at[i])

    def wo_copy(layer, i):
        depth = pl.ds(pl.multiple_of(core * kdim, 128), kdim)
        cols = pl.ds(pl.multiple_of(i * o_chunk, 128), o_chunk)
        return pltpu.make_async_copy(wo_hbm.at[layer, depth, cols], wo.at[i], wo_sem.at[i])

    def cache_copy(layer, b):
        return pltpu.make_async_copy(cache_hbm.at[layer, b], cbuf.at[layer, 2 * core + b], c_sem.at[layer, b])

    def ffn_pairs(layer, k):
        used = pl.ds(0, hid_dim)
        return [
            (wg_hbm.at[layer], wgu.at[layer, 2 * k, used]),
            (wu_hbm.at[layer], wgu.at[layer, 2 * k + 1, used]),
            (wd_hbm.at[layer], wd.at[layer, k])]

    def ffn_copies(layer):
        return [
            pltpu.make_async_copy(src, dst, f_sem.at[layer, i])
            for i, (src, dst) in enumerate(ffn_pairs(layer, core))]

    inputs = [
        pltpu.make_async_copy(src, dst, in_sem.at[i])
        for i, (src, dst) in enumerate(((x_hbm, xin), (len_hbm, lens), (ag_hbm, ag), (fg_hbm, fg)))]
    for copy in inputs:
        copy.start()
    for b in range(2):
        cache_copy(0, b).start()
    for i in range(n_q):
        wq_copy(0, i).start()

    for copy in ffn_copies(0):
        copy.start()
    for i in range(n_o):
        wo_copy(0, i).start()

    barrier = pltpu.get_barrier_semaphore()
    pl.semaphore_signal(barrier, inc=1, device_id=partner, device_id_type=MESH)

    for i, j, k in cube_shifts:
        pl.semaphore_signal(barrier, inc=1, device_id=device(z=i, y=j, x=k), device_id_type=MESH)
    pl.semaphore_wait(barrier, len(cube_shifts) + 1)

    def remote(layer, index, src, dst, peer):
        return pltpu.make_async_remote_copy(
            src_ref=src, dst_ref=dst, send_sem=ssem.at[layer, index], recv_sem=rsem.at[layer, index],
            device_id=peer, device_id_type=MESH)

    def recv(layer, index, dst, peer):
        remote(layer, index, dst, dst, peer).wait_recv()

    def cache_sends(layer):
        return [
            remote(layer, 2 + b, cbuf.at[layer, 2 * core + b] if layer == 0 else cache_hbm.at[layer, b],
                   cbuf.at[layer, 2 * core + b], partner)
            for b in range(2)]

    def ffn_sends(layer):
        return [
            remote(layer, 4 + i, dst if layer == 0 else src, dst, partner)
            for i, (src, dst) in enumerate(ffn_pairs(layer, core))]

    def x_send(layer):
        return remote(layer, 0, xall.at[layer, core], xall.at[layer, core], partner)

    def len_send():
        return remote(0, 7, lbuf.at[core], lbuf.at[core], partner)

    def y_send(layer):
        return remote(layer, 1, ypart.at[layer, other], yrecv.at[layer], partner)

    for copy in inputs:
        copy.wait()
    xall[0, core] = xin[...].astype(F32)
    x_send(0).start()
    for b in range(2):
        lbuf[core, b:b + 1, :] = jnp.full((1, 128), lens[b], jnp.int32).astype(F32)
    len_send().start()
    for b in range(2):
        cache_copy(0, b).wait()
    for copy in cache_sends(0):
        copy.start()

    lhs[4:8, :] = jnp.zeros((4, kdim), F32)
    log = side.bit_length() - 1
    across = lax.broadcasted_iota(jnp.int32, (rows, rows), 1)
    down = lax.broadcasted_iota(jnp.int32, (rows, rows), 0)
    at = {'x': (across >> 1) & (side - 1), 'y': (across >> (1 + log)) & (side - 1), 'z': across >> (1 + 2 * log)}
    for c in (1, 2):
        o, a, b = COLOURS[c]
        place = (((at[o] << (2 * log)) | (at[a] << log) | at[b]) << 1) | (across & 1)
        pick[c - 1] = (place == down).astype(F32).astype(BF16)
    recv(0, 7, lbuf.at[other], partner)

    def rms(v, gain):
        mean_sq = jnp.mean(v * v, axis=-1, keepdims=True)
        return v * lax.rsqrt(mean_sq + NORM_EPS) * gain

    def attention(layer):
        recv(layer, 0, xall.at[layer, other], partner)
        x4 = jnp.concatenate([xall[layer, 0], xall[layer, 1]], axis=0)
        normed = rms(x4, ag[layer:layer + 1, :])
        h8 = jnp.concatenate([normed, normed], axis=0).astype(BF16)

        def q_step(i, carry):
            wq_copy(layer, i).wait()
            qrow[:, pl.ds(pl.multiple_of(i * q_chunk, 128), q_chunk)] = dot(h8, wq[i])
            return carry

        lax.fori_loop(0, n_q, q_step, 0)
        for copy in ffn_copies(layer):
            copy.wait()
        if layer == 0:
            for copy in ffn_sends(0):
                copy.start()
        pair = 2 * kv
        for j in range(heads_half // 2):
            block = qrow[:, j * pair:(j + 1) * pair]
            odd = pltpu.roll(block[:, latent:latent + 640], 640 - 64, 1)
            for parity, q8 in ((0, block[:, :640]), (1, odd)):
                h = 2 * j + parity
                for b in range(4):
                    qbuf[b, h:h + 1, :] = q8[b:b + 1, :]
        positions = lax.broadcasted_iota(jnp.int32, (heads_half, seq), 1).astype(F32)
        for b in range(2):
            if layer:
                cache_copy(layer, b).wait()
            recv(layer, 2 + b, cbuf.at[layer, 2 * other + b], partner)
        for b in range(4):
            q = qbuf[b][:, :kv].astype(BF16)
            s = dot(q, cbuf[layer, b]) * scale
            length = lbuf[b // 2, b % 2:b % 2 + 1, 0:1]
            s = jnp.where(positions < length, s, -jnp.inf)
            e = jnp.exp(s - jnp.max(s, axis=-1, keepdims=True))
            p = (e / jnp.sum(e, axis=-1, keepdims=True)).astype(BF16)
            o = dot_nt(p, cbuf[layer, b, :latent, :])
            for h in range(heads_half):
                lhs[b:b + 1, h * latent:(h + 1) * latent] = o[h:h + 1, :]
        lhs_b = lhs[...].astype(BF16)

        def o_step(i, carry):
            wo_copy(layer, i).wait()
            cols = pl.ds(pl.multiple_of(i * o_chunk, 128), o_chunk)
            y = dot(lhs_b, wo[i])
            ypart[layer, 0, :, cols] = y[0:2]
            ypart[layer, 1, :, cols] = y[2:4]
            return carry

        lax.fori_loop(0, n_o, o_step, 0)

    def prefetch(layer):
        for b in range(2):
            cache_copy(layer, b).start()

        for copy in ffn_copies(layer):
            copy.start()
        for i in range(n_q):
            wq_copy(layer, i).start()
        for i in range(n_o):
            wo_copy(layer, i).start()

    my_slot = coord['y'] * side + coord['x']

    def gather_copy(layer, i, j, k):
        block = gin.at[coord['z'], my_slot]
        return pltpu.make_async_remote_copy(
            src_ref=block, dst_ref=block, send_sem=ag_s.at[layer, i], recv_sem=ag_r.at[layer, i],
            device_id=device(z=i, y=j, x=k), device_id_type=MESH)

    def gather_wait(layer, i):
        part = gin.at[step(coord['z'], side - i)]
        if i == 0:
            part = gin.at[coord['z'], pl.ds(0, plane - 1)]
        return pltpu.make_async_remote_copy(
            src_ref=part, dst_ref=part, send_sem=ag_s.at[layer, i], recv_sem=ag_r.at[layer, i],
            device_id=partner, device_id_type=MESH)

    def slot(c):
        _, a, b = COLOURS[c]
        return coord[a] * side + coord[b]

    def scatter_copy(layer, c, d):
        axis = COLOURS[c][0]
        return remote(layer, 9 + (side - 1) * c + d - 1, s_buf[c].at[step(coord[axis], d)], r1[c].at[d - 1],
                      device(**{axis: d}))

    def plane_copy(layer, c, i, j):
        _, a, b = COLOURS[c]
        target = step(coord[a], i) * side + step(coord[b], j)
        return pltpu.make_async_remote_copy(
            src_ref=u_buf[c].at[target], dst_ref=r2[c].at[slot(c)],
            send_sem=rsp_s.at[layer, c], recv_sem=rsp_r.at[layer, c],
            device_id=device(**{a: i, b: j}), device_id_type=MESH)

    def plane_wait(layer, c):
        part = r2[c].at[pl.ds(0, plane - 1)]
        return pltpu.make_async_remote_copy(
            src_ref=part, dst_ref=part, send_sem=rsp_s.at[layer, c], recv_sem=rsp_r.at[layer, c],
            device_id=partner, device_id_type=MESH)

    def ffn(layer):
        recv(layer, 1, yrecv.at[layer], partner)
        x2 = (xall[layer, core] + (ypart[layer, core] + yrecv[layer])).astype(BF16).astype(F32)
        gin[coord['z'], my_slot] = rms(x2, fg[layer:layer + 1, :]).astype(BF16)
        for shift in cube_shifts:
            gather_copy(layer, *shift).start()
        if layer + 1 < layers:
            for copy in cache_sends(layer + 1) + ffn_sends(layer + 1):
                copy.start()
        for i, (_, dst) in enumerate(ffn_pairs(layer, other)):
            recv(layer, 4 + i, dst, partner)
        for i in axis_shifts + [0]:
            gather_wait(layer, i).wait_recv()
            z = step(coord['z'], side - i)
            for j in range(plane):
                asm[2 * j:2 * j + 2, :] = gin[z, j].astype(F32)
            gu = dot_nt(asm[...].astype(BF16), wgu[layer].reshape(4 * 128, d_model))
            for k in range(2):
                gate, up = gu[:, 256 * k:256 * k + 128], gu[:, 256 * k + 128:256 * k + 256]
                hid[k, pl.ds(pl.multiple_of(z * group, 16), group), :] = (jax.nn.silu(gate) * up).astype(BF16)

        for c, (base, width) in enumerate(columns):
            total = None
            for k in range(2):
                a = hid[k][:, :hid_dim]
                if c:
                    a = dot(pick[c - 1], a).astype(BF16)
                term = dot(a, wd[layer, k, :, base:base + width])
                total = term if total is None else total + term
            s_buf[c][...] = total.reshape(side, group, width)
            for d in axis_shifts:
                scatter_copy(layer, c, d).start()
        for c in range(3):
            axis, a, b = COLOURS[c]
            total = s_buf[c][coord[axis]]
            for d in axis_shifts:
                recv(layer, 9 + (side - 1) * c + d - 1, r1[c].at[d - 1], device(**{axis: d}))
                total = total + r1[c][d - 1]
            for i in range(plane):
                u_buf[c][i] = total[2 * i:2 * i + 2]
            for i, j in plane_shifts:
                plane_copy(layer, c, i, j).start()
        sums = []
        for c in range(3):
            r2[c][slot(c)] = u_buf[c][slot(c)]
            plane_wait(layer, c).wait_recv()
            total = r2[c][0]
            for i in range(1, plane):
                total = total + r2[c][i]
            sums.append(total)
        x2 = (x2 + jnp.concatenate(sums, axis=1)).astype(BF16).astype(F32)
        if layer + 1 < layers:
            xall[layer + 1, core] = x2
            x_send(layer + 1).start()
        else:
            out_ref[...] = x2
        for i in range(side):
            gather_wait(layer, i).wait_send()
        for c in range(3):
            plane_wait(layer, c).wait_send()
            for d in axis_shifts:
                scatter_copy(layer, c, d).wait_send()

    for layer in range(layers):
        attention(layer)
        y_send(layer).start()
        if layer + 1 < layers:
            prefetch(layer + 1)
        ffn(layer)
    len_send().wait_send()
    for layer in range(layers):
        for copy in [x_send(layer), y_send(layer)] + cache_sends(layer) + ffn_sends(layer):
            copy.wait_send()


def solution(mesh):
    devices = mesh.shape['dp']
    side = round((devices // 2) ** (1 / 3))

    def local_step(x, lengths, cache, attn_gain, ffn_gain, w_query, w_attn_out, w_up, w_gate, w_down):
        layers, _, seq, kv = cache.shape
        d_model = x.shape[1]
        heads = w_query.shape[2] // kv
        latent = w_attn_out.shape[1] // heads
        hid_dim = w_up.shape[2]
        hh = heads // 2
        q_chunk, o_chunk = 512, 256
        n_q, n_o = hh * kv // q_chunk, d_model // o_chunk
        plane = side * side
        group = 2 * plane
        rows = group * side
        widths = [w for _, w in colour_columns(d_model)]
        cfg = (side, layers, heads, kv, latent, seq, d_model, hid_dim, q_chunk, o_chunk)
        hbm = pl.BlockSpec(memory_space=pl.ANY)
        scratch = [
            pltpu.VMEM((n_q, d_model, q_chunk), BF16),
            pltpu.VMEM((n_o, hh * latent, o_chunk), BF16),
            pltpu.VMEM((layers, 4, kv, seq), BF16),
            pltpu.VMEM((layers, 4, 128, d_model), BF16),
            pltpu.VMEM((layers, 2, hid_dim, d_model), BF16),
            pltpu.VMEM((2, d_model), BF16),
            pltpu.SMEM((2,), jnp.int32),
            pltpu.VMEM((layers, d_model), F32),
            pltpu.VMEM((layers, d_model), F32),
            pltpu.VMEM((2, 2, 128), F32),
            pltpu.VMEM((layers, 2, 2, d_model), F32),
            pltpu.VMEM((8, hh * kv), F32),
            pltpu.VMEM((4, hh, 640), F32),
            pltpu.VMEM((8, hh * latent), F32),
            pltpu.VMEM((layers, 2, 2, d_model), F32),
            pltpu.VMEM((layers, 2, d_model), F32),
            pltpu.VMEM((group, d_model), F32),
            pltpu.VMEM((2, rows, 128), BF16),
            pltpu.VMEM((2, rows, rows), BF16),
            pltpu.VMEM((side, plane, 2, d_model), BF16),
            *[pltpu.VMEM((side, group, w), F32) for w in widths],
            *[pltpu.VMEM((side - 1, group, w), F32) for w in widths],
            *[pltpu.VMEM((plane, 2, w), F32) for w in widths],
            *[pltpu.VMEM((plane, 2, w), F32) for w in widths],
            pltpu.SemaphoreType.DMA((n_q,)),
            pltpu.SemaphoreType.DMA((n_o,)),
            pltpu.SemaphoreType.DMA((layers, 2)),
            pltpu.SemaphoreType.DMA((layers, 3)),
            pltpu.SemaphoreType.DMA((4,)),
            pltpu.SemaphoreType.DMA((layers, 18)),
            pltpu.SemaphoreType.DMA((layers, 18)),
            pltpu.SemaphoreType.DMA((layers, side)),
            pltpu.SemaphoreType.DMA((layers, side)),
            pltpu.SemaphoreType.DMA((layers, 3)),
            pltpu.SemaphoreType.DMA((layers, 3)),
        ]
        out = pl.pallas_call(
            functools.partial(kernel, cfg),
            out_shape=pltpu.VMEM(x.shape, F32),
            in_specs=[hbm] * 10,
            out_specs=pl.BlockSpec(memory_space=pltpu.VMEM),
            scratch_shapes=scratch,
            compiler_params=pltpu.CompilerParams(
                collective_id=0, has_side_effects=True, vmem_limit_bytes=66_500_000),
            name='mla_decode',
        )(x, lengths, attn_gain, ffn_gain, jnp.swapaxes(cache, 2, 3), w_query, w_attn_out,
          jnp.swapaxes(w_up, 1, 2), jnp.swapaxes(w_gate, 1, 2), w_down)
        return out.astype(BF16)

    rows = ('replica', 'dp')
    return jax.shard_map(
        local_step,
        mesh=mesh,
        in_specs=(P(rows, None), P(rows), P(None, rows, None, None), P(), P(), P(), P(),
                  P(None, None, 'dp'), P(None, None, 'dp'), P(None, 'dp', None)),
        out_specs=P(rows, None),
        check_vma=False,
    )
```

```python
import functools

import jax
import jax.numpy as jnp
from jax import lax
from jax.experimental import pallas as pl
from jax.experimental.pallas import tpu as pltpu
from jax.sharding import PartitionSpec as P

NORM_EPS = 1e-6
MESH = pl.DeviceIdType.MESH
F32 = jnp.float32
BF16 = jnp.bfloat16
COLOURS = (('z', 'y', 'x'), ('x', 'z', 'y'), ('y', 'z', 'x'))


def dot(a, b):
    return jnp.dot(a, b, preferred_element_type=F32)


def dot_nt(a, b):
    return lax.dot_general(a, b, (((1,), (1,)), ((), ())), preferred_element_type=F32)


def colour_columns(d_model):
    tiles = d_model // 128
    widths = [128 * ((tiles + 2 - c) // 3) for c in range(3)]
    return [(sum(widths[:c]), widths[c]) for c in range(3)]


def kernel(
    cfg,
    x_hbm, len_hbm, ag_hbm, fg_hbm, cache_hbm, wq_hbm, wo_hbm, wu_hbm, wg_hbm, wd_hbm,
    out_ref,
    wq, wo, cbuf, wu, wg, wd,
    xin, lens, ag, fg, xsend, xrecv, qrow, qsend, qbuf, obuf, osend, orecv, lhs, ysend, yrecv, asm,
    p1a, p1b, p1c, g_a, g_b, g_c, s_a, s_b, s_c, r1a, r1b, r1c, u_a, u_b, u_c, r2a, r2b, r2c,
    wq_sem, wo_sem, c_sem, f_sem, in_sem, ssem, rsem, agp_s, agp_r, rsp_s, rsp_r,
):
    side, layers, heads, kv, latent, seq, d_model, q_chunk, o_chunk = cfg
    heads_half = heads // 2
    qw = heads_half * kv
    n_q = qw // q_chunk
    n_o = d_model // o_chunk
    kdim = heads_half * latent
    plane = side * side
    rows = 2 * side ** 3
    scale = (3 * (kv - latent)) ** -0.5
    columns = colour_columns(d_model)
    p1, g_buf, s_buf = (p1a, p1b, p1c), (g_a, g_b, g_c), (s_a, s_b, s_c)
    r1, u_buf, r2 = (r1a, r1b, r1c), (u_a, u_b, u_c), (r2a, r2b, r2c)

    me = lax.axis_index('dp')
    core = lax.rem(me, 2)
    chip = lax.div(me, 2)
    coord = {'x': lax.rem(chip, side), 'y': lax.rem(lax.div(chip, side), side), 'z': lax.div(chip, plane)}
    other = 1 - core

    def step(c, d):
        return lax.rem(c + d, side)

    def device(k=core, **shift):
        at = {a: step(coord[a], shift.get(a, 0)) for a in 'zyx'}
        return {'dp': ((at['z'] * side + at['y']) * side + at['x']) * 2 + k}

    partner = {'dp': chip * 2 + other}
    hops = lambda d: min(d, side - d)
    axis_shifts = sorted(range(1, side), key=hops, reverse=True)
    plane_shifts = sorted(
        [(i, j) for i in range(side) for j in range(side) if i or j],
        key=lambda s: hops(s[0]) + hops(s[1]), reverse=True)

    def wq_copy(layer, i):
        cols = pl.ds(pl.multiple_of(core * qw + i * q_chunk, 128), q_chunk)
        return pltpu.make_async_copy(wq_hbm.at[layer, :, cols], wq.at[i], wq_sem.at[i])

    def wo_copy(layer, i):
        depth = pl.ds(pl.multiple_of(core * kdim, 128), kdim)
        cols = pl.ds(pl.multiple_of(i * o_chunk, 128), o_chunk)
        return pltpu.make_async_copy(wo_hbm.at[layer, depth, cols], wo.at[i], wo_sem.at[i])

    def cache_copy(layer, b):
        return pltpu.make_async_copy(cache_hbm.at[layer, b], cbuf.at[layer, b], c_sem.at[layer, b])

    ffn_pairs = ((wg_hbm, wg), (wu_hbm, wu), (wd_hbm, wd))

    def ffn_copies(layer):
        return [
            pltpu.make_async_copy(src.at[layer], dst.at[layer, core], f_sem.at[layer, i])
            for i, (src, dst) in enumerate(ffn_pairs)]

    inputs = [
        pltpu.make_async_copy(src, dst, in_sem.at[i])
        for i, (src, dst) in enumerate(((x_hbm, xin), (len_hbm, lens), (ag_hbm, ag), (fg_hbm, fg)))]
    for copy in inputs:
        copy.start()
    for i in range(n_q):
        wq_copy(0, i).start()
    for b in range(2):
        cache_copy(0, b).start()
    for copy in ffn_copies(0):
        copy.start()
    for i in range(n_o):
        wo_copy(0, i).start()

    barrier = pltpu.get_barrier_semaphore()
    peers = [partner] + [
        device(**shift) for shift in
        [{a: d} for a in 'zyx' for d in range(1, side)]
        + [{a: d, b: e} for a, b in ('zy', 'zx', 'yx') for d in range(1, side) for e in range(1, side)]]
    for peer in peers:
        pl.semaphore_signal(barrier, inc=1, device_id=peer, device_id_type=MESH)
    pl.semaphore_wait(barrier, len(peers))

    pending = []

    def remote(layer, index, src, dst, peer):
        return pltpu.make_async_remote_copy(
            src_ref=src, dst_ref=dst, send_sem=ssem.at[layer, index], recv_sem=rsem.at[layer, index],
            device_id=peer, device_id_type=MESH)

    def send(layer, index, src, dst, peer):
        copy = remote(layer, index, src, dst, peer)
        copy.start()
        pending.append(copy)

    def recv(layer, index, dst, peer):
        remote(layer, index, dst, dst, peer).wait_recv()

    def send_ffn(layer, which):
        for i in which:
            src, dst = ffn_pairs[i]
            send(layer, 4 + i, src.at[layer], dst.at[layer, core], partner)

    for copy in inputs:
        copy.wait()
    xsend[0] = xin[...].astype(F32)
    send(0, 0, xsend.at[0], xrecv.at[0], partner)
    send_ffn(0, (0, 1))
    lhs[4:8, :] = jnp.zeros((4, kdim), F32)

    def rms(v, gain):
        mean_sq = jnp.mean(v * v, axis=-1, keepdims=True)
        return v * lax.rsqrt(mean_sq + NORM_EPS) * gain

    def attention(layer, x2):
        recv(layer, 0, xrecv.at[layer], partner)
        x4 = jnp.concatenate([x2, xrecv[layer]], axis=0)
        normed = rms(x4, ag[layer:layer + 1, :])
        h8 = jnp.concatenate([normed, normed], axis=0).astype(BF16)

        def q_step(i, carry):
            wq_copy(layer, i).wait()
            qrow[:, pl.ds(pl.multiple_of(i * q_chunk, 128), q_chunk)] = dot(h8, wq[i])
            return carry

        lax.fori_loop(0, n_q, q_step, 0)
        for copy in ffn_copies(layer):
            copy.wait()
        pair = 2 * kv
        for j in range(heads_half // 2):
            block = qrow[:, j * pair:(j + 1) * pair]
            odd = pltpu.roll(block[:, latent:latent + 640], 640 - 64, 1)
            for parity, q8 in ((0, block[:, :640]), (1, odd)):
                h = 2 * j + parity
                for b in range(2):
                    qbuf[layer, core, b, h:h + 1, :] = q8[b:b + 1, :]
                    qsend[layer, b, h:h + 1, :] = q8[2 + b:3 + b, :]
        send(layer, 2, qsend.at[layer], qbuf.at[layer, core], partner)
        positions = lax.broadcasted_iota(jnp.int32, (heads, seq), 1)
        for b in range(2):
            cache_copy(layer, b).wait()
        recv(layer, 2, qbuf.at[layer, other], partner)
        for b in range(2):
            q = jnp.concatenate([qbuf[layer, 0, b], qbuf[layer, 1, b]], axis=0)[:, :kv].astype(BF16)
            s = dot(q, cbuf[layer, b]) * scale
            s = jnp.where(positions < lens[b], s, -jnp.inf)
            e = jnp.exp(s - jnp.max(s, axis=-1, keepdims=True))
            p = (e / jnp.sum(e, axis=-1, keepdims=True)).astype(BF16)
            o = dot_nt(p, cbuf[layer, b, :latent, :])
            obuf[b, 0] = o[:heads_half]
            obuf[b, 1] = o[heads_half:]
        for b in range(2):
            theirs = obuf[b, other]
            for h in range(heads_half):
                osend[layer, b:b + 1, h * latent:(h + 1) * latent] = theirs[h:h + 1, :]
        send(layer, 3, osend.at[layer], orecv.at[layer], partner)
        for b in range(2):
            mine = obuf[b, core]
            for h in range(heads_half):
                lhs[b:b + 1, h * latent:(h + 1) * latent] = mine[h:h + 1, :]
        recv(layer, 3, orecv.at[layer], partner)
        lhs[2:4, :] = orecv[layer]
        lhs_b = lhs[...].astype(BF16)

        def o_step(i, carry):
            wo_copy(layer, i).wait()
            y = dot(lhs_b, wo[i])
            cols = pl.ds(pl.multiple_of(i * o_chunk, 128), o_chunk)
            ysend[layer, 0, :, cols] = y[0:2]
            ysend[layer, 1, :, cols] = y[2:4]
            return carry

        lax.fori_loop(0, n_o, o_step, 0)
        send(layer, 1, ysend.at[layer, 1], yrecv.at[layer], partner)
        if layer == 0:
            send_ffn(0, (2,))
        if layer + 1 < layers:
            for b in range(2):
                cache_copy(layer + 1, b).start()
            for copy in ffn_copies(layer + 1):
                copy.start()
            for i in range(n_q):
                wq_copy(layer + 1, i).start()
            for i in range(n_o):
                wo_copy(layer + 1, i).start()
        recv(layer, 1, yrecv.at[layer], partner)
        return (x2 + (ysend[layer, 0] + yrecv[layer])).astype(BF16).astype(F32)

    def slot(c):
        _, a, b = COLOURS[c]
        return coord[a] * side + coord[b]

    def plane_wait(buf, layer, send_sem, recv_sem, c, sent):
        part = buf.at[layer, pl.ds(0, plane - 1)]
        copy = pltpu.make_async_remote_copy(
            src_ref=part, dst_ref=part, send_sem=send_sem.at[layer, c], recv_sem=recv_sem.at[layer, c],
            device_id=partner, device_id_type=MESH)
        return copy.wait_send() if sent else copy.wait_recv()

    def natural_of(index):
        log = side.bit_length() - 1
        r = index & 1
        at = {'x': (index >> 1) & (side - 1), 'y': (index >> (1 + log)) & (side - 1), 'z': index >> (1 + 2 * log)}
        return [
            (((at[o] << (2 * log)) | (at[a] << log) | at[b]) << 1) | r for o, a, b in COLOURS]

    def ffn(layer, x2):
        g2 = rms(x2, fg[layer:layer + 1, :]).astype(BF16)
        for c, (base, width) in enumerate(columns):
            _, a, b = COLOURS[c]
            p1[c][layer, slot(c)] = g2[:, base:base + width]
            for i, j in plane_shifts:
                block = p1[c].at[layer, slot(c)]
                pltpu.make_async_remote_copy(
                    src_ref=block, dst_ref=block, send_sem=agp_s.at[layer, c], recv_sem=agp_r.at[layer, c],
                    device_id=device(**{a: i, b: j}), device_id_type=MESH).start()
        if layer + 1 < layers:
            send_ffn(layer + 1, (0, 1, 2))
        for c, (base, width) in enumerate(columns):
            axis = COLOURS[c][0]
            plane_wait(p1[c], layer, agp_s, agp_r, c, False)
            for i in range(plane):
                asm[2 * i:2 * i + 2, base:base + width] = p1[c][layer, i].astype(F32)
            g_buf[c][layer, coord[axis]] = asm[:, base:base + width].astype(BF16)
            own = g_buf[c].at[layer, coord[axis]]
            for d in axis_shifts:
                send(layer, 8 + 3 * c + d - 1, own, own, device(**{axis: d}))
        for i, (_, dst) in enumerate(ffn_pairs):
            recv(layer, 4 + i, dst.at[layer, other], partner)

        across = lax.broadcasted_iota(jnp.int32, (rows, rows), 1)
        down = lax.broadcasted_iota(jnp.int32, (rows, rows), 0)
        parts = []
        for c, (base, width) in enumerate(columns):
            axis = COLOURS[c][0]
            for d in axis_shifts:
                recv(layer, 8 + 3 * c + d - 1, g_buf[c].at[layer, step(coord[axis], side - d)], device(**{axis: d}))
            part = g_buf[c][layer].reshape(rows, width)
            if c:
                pick = (natural_of(down)[c] == across).astype(F32).astype(BF16)
                part = dot(pick, part).astype(BF16)
            parts.append(part)
        g = jnp.concatenate(parts, axis=1)
        hidden = []
        for k in range(2):
            gate = dot_nt(g, wg[layer, k])
            up = dot_nt(g, wu[layer, k])
            hidden.append((jax.nn.silu(gate) * up).astype(BF16))

        for c, (base, width) in enumerate(columns):
            axis = COLOURS[c][0]
            total = None
            for k in range(2):
                a = hidden[k]
                if c:
                    pick = (natural_of(across)[c] == down).astype(F32).astype(BF16)
                    a = dot(pick, a).astype(BF16)
                term = dot(a, wd[layer, k, :, base:base + width])
                total = term if total is None else total + term
            s_buf[c][layer] = total.reshape(side, 2 * plane, width)
            for d in axis_shifts:
                send(layer, 17 + 3 * c + d - 1, s_buf[c].at[layer, step(coord[axis], d)], r1[c].at[layer, d - 1],
                     device(**{axis: d}))
        for c, (base, width) in enumerate(columns):
            axis, a, b = COLOURS[c]
            total = s_buf[c][layer, coord[axis]]
            for d in axis_shifts:
                recv(layer, 17 + 3 * c + d - 1, r1[c].at[layer, d - 1], device(**{axis: d}))
                total = total + r1[c][layer, d - 1]
            for i in range(plane):
                u_buf[c][layer, i] = total[2 * i:2 * i + 2]
            for i, j in plane_shifts:
                target = step(coord[a], i) * side + step(coord[b], j)
                pltpu.make_async_remote_copy(
                    src_ref=u_buf[c].at[layer, target], dst_ref=r2[c].at[layer, slot(c)],
                    send_sem=rsp_s.at[layer, c], recv_sem=rsp_r.at[layer, c],
                    device_id=device(**{a: i, b: j}), device_id_type=MESH).start()
        sums = []
        for c in range(3):
            r2[c][layer, slot(c)] = u_buf[c][layer, slot(c)]
            plane_wait(r2[c], layer, rsp_s, rsp_r, c, False)
            total = r2[c][layer, 0]
            for i in range(1, plane):
                total = total + r2[c][layer, i]
            sums.append(total)
        return (x2 + jnp.concatenate(sums, axis=1)).astype(BF16).astype(F32)

    x2 = xsend[0]
    for layer in range(layers):
        x2 = attention(layer, x2)
        x2 = ffn(layer, x2)
        if layer + 1 < layers:
            xsend[layer + 1] = x2
            send(layer + 1, 0, xsend.at[layer + 1], xrecv.at[layer + 1], partner)
    out_ref[...] = x2
    for copy in pending:
        copy.wait_send()
    for layer in range(layers):
        for c in range(3):
            plane_wait(p1[c], layer, agp_s, agp_r, c, True)
            plane_wait(u_buf[c], layer, rsp_s, rsp_r, c, True)


def solution(mesh):
    devices = mesh.shape['dp']
    side = round((devices // 2) ** (1 / 3))

    def local_step(x, lengths, cache, attn_gain, ffn_gain, w_query, w_attn_out, w_up, w_gate, w_down):
        layers, _, seq, kv = cache.shape
        d_model = x.shape[1]
        heads = w_query.shape[2] // kv
        latent = w_attn_out.shape[1] // heads
        hid = w_up.shape[2]
        hh = heads // 2
        q_chunk, o_chunk = 512, 256
        n_q, n_o = hh * kv // q_chunk, d_model // o_chunk
        plane = side * side
        widths = [w for _, w in colour_columns(d_model)]
        cfg = (side, layers, heads, kv, latent, seq, d_model, q_chunk, o_chunk)
        hbm = pl.BlockSpec(memory_space=pl.ANY)
        scratch = [
            pltpu.VMEM((n_q, d_model, q_chunk), BF16),
            pltpu.VMEM((n_o, hh * latent, o_chunk), BF16),
            pltpu.VMEM((layers, 2, kv, seq), BF16),
            pltpu.VMEM((layers, 2, hid, d_model), BF16),
            pltpu.VMEM((layers, 2, hid, d_model), BF16),
            pltpu.VMEM((layers, 2, hid, d_model), BF16),
            pltpu.VMEM((2, d_model), BF16),
            pltpu.SMEM((2,), jnp.int32),
            pltpu.VMEM((layers, d_model), F32),
            pltpu.VMEM((layers, d_model), F32),
            pltpu.VMEM((layers, 2, d_model), F32),
            pltpu.VMEM((layers, 2, d_model), F32),
            pltpu.VMEM((8, hh * kv), F32),
            pltpu.VMEM((layers, 2, hh, 640), F32),
            pltpu.VMEM((layers, 2, 2, hh, 640), F32),
            pltpu.VMEM((2, 2, hh, latent), F32),
            pltpu.VMEM((layers, 2, hh * latent), F32),
            pltpu.VMEM((layers, 2, hh * latent), F32),
            pltpu.VMEM((8, hh * latent), F32),
            pltpu.VMEM((layers, 2, 2, d_model), F32),
            pltpu.VMEM((layers, 2, d_model), F32),
            pltpu.VMEM((2 * plane, d_model), F32),
            *[pltpu.VMEM((layers, plane, 2, w), BF16) for w in widths],
            *[pltpu.VMEM((layers, side, 2 * plane, w), BF16) for w in widths],
            *[pltpu.VMEM((layers, side, 2 * plane, w), F32) for w in widths],
            *[pltpu.VMEM((layers, side - 1, 2 * plane, w), F32) for w in widths],
            *[pltpu.VMEM((layers, plane, 2, w), F32) for w in widths],
            *[pltpu.VMEM((layers, plane, 2, w), F32) for w in widths],
            pltpu.SemaphoreType.DMA((n_q,)),
            pltpu.SemaphoreType.DMA((n_o,)),
            pltpu.SemaphoreType.DMA((layers, 2)),
            pltpu.SemaphoreType.DMA((layers, 3)),
            pltpu.SemaphoreType.DMA((4,)),
            pltpu.SemaphoreType.DMA((layers, 26)),
            pltpu.SemaphoreType.DMA((layers, 26)),
            *[pltpu.SemaphoreType.DMA((layers, 3)) for _ in range(4)],
        ]
        out = pl.pallas_call(
            functools.partial(kernel, cfg),
            out_shape=pltpu.VMEM(x.shape, F32),
            in_specs=[hbm] * 10,
            out_specs=pl.BlockSpec(memory_space=pltpu.VMEM),
            scratch_shapes=scratch,
            compiler_params=pltpu.CompilerParams(
                collective_id=0, has_side_effects=True, vmem_limit_bytes=66_500_000),
            name='mla_decode',
        )(x, lengths, attn_gain, ffn_gain, jnp.swapaxes(cache, 2, 3), w_query, w_attn_out,
          jnp.swapaxes(w_up, 1, 2), jnp.swapaxes(w_gate, 1, 2), w_down)
        return out.astype(BF16)

    rows = ('replica', 'dp')
    return jax.shard_map(
        local_step,
        mesh=mesh,
        in_specs=(P(rows, None), P(rows), P(None, rows, None, None), P(), P(), P(), P(),
                  P(None, None, 'dp'), P(None, None, 'dp'), P(None, 'dp', None)),
        out_specs=P(rows, None),
        check_vma=False,
    )
```

```python
import functools

import jax
import jax.numpy as jnp
from jax import lax
from jax.experimental import pallas as pl
from jax.experimental.pallas import tpu as pltpu
from jax.sharding import PartitionSpec as P

NORM_EPS = 1e-6
MESH = pl.DeviceIdType.MESH
F32 = jnp.float32
BF16 = jnp.bfloat16
COLOURS = (('z', 'y', 'x'), ('x', 'z', 'y'), ('y', 'z', 'x'))


def dot(a, b):
    return jnp.dot(a, b, preferred_element_type=F32)


def dot_nt(a, b):
    return lax.dot_general(a, b, (((1,), (1,)), ((), ())), preferred_element_type=F32)


def colour_columns(d_model):
    tiles = d_model // 128
    widths = [128 * ((tiles + 2 - c) // 3) for c in range(3)]
    return [(sum(widths[:c]), widths[c]) for c in range(3)]


def kernel(
    cfg,
    x_hbm, len_hbm, ag_hbm, fg_hbm, cache_hbm, wq_hbm, wo_hbm, wu_hbm, wg_hbm, wd_hbm,
    out_ref,
    wq, wo, cbuf, wu, wg, wd,
    xin, lens, ag, fg, lbuf, xsend, xrecv, qrow, qbuf, lhs, ysend, yrecv, asm,
    p1a, p1b, p1c, g_a, g_b, g_c, s_a, s_b, s_c, r1a, r1b, r1c, u_a, u_b, u_c, r2a, r2b, r2c,
    wq_sem, wo_sem, c_sem, f_sem, in_sem, ssem, rsem, agp_s, agp_r, rsp_s, rsp_r,
):
    side, layers, heads, kv, latent, seq, d_model, q_chunk, o_chunk = cfg
    heads_half = heads // 2
    qw = heads_half * kv
    n_q = qw // q_chunk
    n_o = d_model // o_chunk
    kdim = heads_half * latent
    early = n_o - 3
    plane = side * side
    rows = 2 * side ** 3
    scale = (3 * (kv - latent)) ** -0.5
    columns = colour_columns(d_model)
    p1, g_buf, s_buf = (p1a, p1b, p1c), (g_a, g_b, g_c), (s_a, s_b, s_c)
    r1, u_buf, r2 = (r1a, r1b, r1c), (u_a, u_b, u_c), (r2a, r2b, r2c)

    me = lax.axis_index('dp')
    core = lax.rem(me, 2)
    chip = lax.div(me, 2)
    coord = {'x': lax.rem(chip, side), 'y': lax.rem(lax.div(chip, side), side), 'z': lax.div(chip, plane)}
    other = 1 - core

    def step(c, d):
        return lax.rem(c + d, side)

    def device(k=core, **shift):
        at = {a: step(coord[a], shift.get(a, 0)) for a in 'zyx'}
        return {'dp': ((at['z'] * side + at['y']) * side + at['x']) * 2 + k}

    partner = {'dp': chip * 2 + other}
    hops = lambda d: min(d, side - d)
    axis_shifts = sorted(range(1, side), key=hops, reverse=True)
    plane_shifts = sorted(
        [(i, j) for i in range(side) for j in range(side) if i or j],
        key=lambda s: hops(s[0]) + hops(s[1]), reverse=True)

    def wq_copy(layer, i):
        cols = pl.ds(pl.multiple_of(core * qw + i * q_chunk, 128), q_chunk)
        return pltpu.make_async_copy(wq_hbm.at[layer, :, cols], wq.at[i], wq_sem.at[i])

    def wo_copy(layer, i):
        depth = pl.ds(pl.multiple_of(core * kdim, 128), kdim)
        cols = pl.ds(pl.multiple_of(i * o_chunk, 128), o_chunk)
        return pltpu.make_async_copy(wo_hbm.at[layer, depth, cols], wo.at[i], wo_sem.at[i])

    def cache_copy(layer, b):
        return pltpu.make_async_copy(cache_hbm.at[layer, b], cbuf.at[layer, b], c_sem.at[layer, b])

    ffn_pairs = ((wg_hbm, wg), (wu_hbm, wu), (wd_hbm, wd))

    def ffn_copies(layer):
        return [
            pltpu.make_async_copy(src.at[layer], dst.at[layer, core], f_sem.at[layer, i])
            for i, (src, dst) in enumerate(ffn_pairs)]

    inputs = [
        pltpu.make_async_copy(src, dst, in_sem.at[i])
        for i, (src, dst) in enumerate(((x_hbm, xin), (len_hbm, lens), (ag_hbm, ag), (fg_hbm, fg)))]
    for copy in inputs:
        copy.start()
    for b in range(2):
        cache_copy(0, b).start()
    for i in range(n_q):
        wq_copy(0, i).start()

    barrier = pltpu.get_barrier_semaphore()
    peers = [partner] + [
        device(**shift) for shift in
        [{a: d} for a in 'zyx' for d in range(1, side)]
        + [{a: d, b: e} for a, b in ('zy', 'zx', 'yx') for d in range(1, side) for e in range(1, side)]]
    for peer in peers:
        pl.semaphore_signal(barrier, inc=1, device_id=peer, device_id_type=MESH)
    pl.semaphore_wait(barrier, len(peers))

    pending = []

    def remote(layer, index, src, dst, peer):
        return pltpu.make_async_remote_copy(
            src_ref=src, dst_ref=dst, send_sem=ssem.at[layer, index], recv_sem=rsem.at[layer, index],
            device_id=peer, device_id_type=MESH)

    def send(layer, index, src, dst, peer):
        copy = remote(layer, index, src, dst, peer)
        copy.start()
        pending.append(copy)

    def recv(layer, index, dst, peer):
        remote(layer, index, dst, dst, peer).wait_recv()

    def send_cache(layer, src):
        for b in range(2):
            send(layer, 2 + b, src.at[layer, b], cbuf.at[layer, 2 + b], partner)

    def send_ffn(layer, local):
        for i, (src, dst) in enumerate(ffn_pairs):
            src = dst.at[layer, core] if local else src.at[layer]
            send(layer, 4 + i, src, dst.at[layer, core], partner)

    for copy in inputs:
        copy.wait()
    xsend[0] = xin[...].astype(F32)
    send(0, 0, xsend.at[0], xrecv.at[0], partner)
    for b in range(2):
        lbuf[0, b:b + 1, :] = jnp.full((1, 128), lens[b], jnp.int32).astype(F32)
    send(0, 7, lbuf.at[0], lbuf.at[1], partner)
    for b in range(2):
        cache_copy(0, b).wait()
    send_cache(0, cbuf)
    lhs[4:8, :] = jnp.zeros((4, kdim), F32)

    def rms(v, gain):
        mean_sq = jnp.mean(v * v, axis=-1, keepdims=True)
        return v * lax.rsqrt(mean_sq + NORM_EPS) * gain

    def attention(layer, x2):
        recv(layer, 0, xrecv.at[layer], partner)
        if layer == 0:
            recv(0, 7, lbuf.at[1], partner)
        x4 = jnp.concatenate([x2, xrecv[layer]], axis=0)
        normed = rms(x4, ag[layer:layer + 1, :])
        h8 = jnp.concatenate([normed, normed], axis=0).astype(BF16)

        def q_step(i, carry):
            wq_copy(layer, i).wait()
            if layer == 0:
                @pl.when(i < early)
                def _():
                    wo_copy(layer, i).start()
            qrow[:, pl.ds(pl.multiple_of(i * q_chunk, 128), q_chunk)] = dot(h8, wq[i])
            return carry

        lax.fori_loop(0, n_q, q_step, 0)
        pair = 2 * kv
        for j in range(heads_half // 2):
            block = qrow[:, j * pair:(j + 1) * pair]
            odd = pltpu.roll(block[:, latent:latent + 640], 640 - 64, 1)
            for parity, q8 in ((0, block[:, :640]), (1, odd)):
                h = 2 * j + parity
                for b in range(4):
                    qbuf[b, h:h + 1, :] = q8[b:b + 1, :]
        positions = lax.broadcasted_iota(jnp.int32, (heads_half, seq), 1).astype(F32)
        if layer:
            for b in range(2):
                cache_copy(layer, b).wait()
        for b in range(2):
            recv(layer, 2 + b, cbuf.at[layer, 2 + b], partner)
        for b in range(4):
            q = qbuf[b][:, :kv].astype(BF16)
            s = dot(q, cbuf[layer, b]) * scale
            length = lbuf[b // 2, b % 2:b % 2 + 1, 0:1]
            s = jnp.where(positions < length, s, -jnp.inf)
            e = jnp.exp(s - jnp.max(s, axis=-1, keepdims=True))
            p = (e / jnp.sum(e, axis=-1, keepdims=True)).astype(BF16)
            o = dot_nt(p, cbuf[layer, b, :latent, :])
            for h in range(heads_half):
                lhs[b:b + 1, h * latent:(h + 1) * latent] = o[h:h + 1, :]
            if layer == 0 and b and early + b - 1 < n_o:
                wo_copy(layer, early + b - 1).start()
                if b == 3:
                    for copy in ffn_copies(layer):
                        copy.start()
        lhs_b = lhs[...].astype(BF16)

        def o_step(i, carry):
            wo_copy(layer, i).wait()
            y = dot(lhs_b, wo[i])
            cols = pl.ds(pl.multiple_of(i * o_chunk, 128), o_chunk)
            ysend[layer, 0, :, cols] = y[0:2]
            ysend[layer, 1, :, cols] = y[2:4]
            return carry

        lax.fori_loop(0, n_o, o_step, 0)
        send(layer, 1, ysend.at[layer, 1], yrecv.at[layer], partner)
        for copy in ffn_copies(layer):
            copy.wait()
        if layer == 0:
            send_ffn(layer, True)
        if layer + 1 < layers:
            for b in range(2):
                cache_copy(layer + 1, b).start()
            for copy in ffn_copies(layer + 1):
                copy.start()
            for i in range(n_q):
                wq_copy(layer + 1, i).start()
            for i in range(n_o):
                wo_copy(layer + 1, i).start()
        recv(layer, 1, yrecv.at[layer], partner)
        return (x2 + (ysend[layer, 0] + yrecv[layer])).astype(BF16).astype(F32)

    def slot(c):
        _, a, b = COLOURS[c]
        return coord[a] * side + coord[b]

    def plane_wait(buf, layer, send_sem, recv_sem, c, sent):
        part = buf.at[layer, pl.ds(0, plane - 1)]
        copy = pltpu.make_async_remote_copy(
            src_ref=part, dst_ref=part, send_sem=send_sem.at[layer, c], recv_sem=recv_sem.at[layer, c],
            device_id=partner, device_id_type=MESH)
        return copy.wait_send() if sent else copy.wait_recv()

    def natural_of(index):
        log = side.bit_length() - 1
        r = index & 1
        at = {'x': (index >> 1) & (side - 1), 'y': (index >> (1 + log)) & (side - 1), 'z': index >> (1 + 2 * log)}
        return [
            (((at[o] << (2 * log)) | (at[a] << log) | at[b]) << 1) | r for o, a, b in COLOURS]

    def ffn(layer, x2):
        g2 = rms(x2, fg[layer:layer + 1, :]).astype(BF16)
        for c, (base, width) in enumerate(columns):
            _, a, b = COLOURS[c]
            p1[c][layer, slot(c)] = g2[:, base:base + width]
            for i, j in plane_shifts:
                block = p1[c].at[layer, slot(c)]
                pltpu.make_async_remote_copy(
                    src_ref=block, dst_ref=block, send_sem=agp_s.at[layer, c], recv_sem=agp_r.at[layer, c],
                    device_id=device(**{a: i, b: j}), device_id_type=MESH).start()
        if layer + 1 < layers:
            send_cache(layer + 1, cache_hbm)
            send_ffn(layer + 1, False)
        for c, (base, width) in enumerate(columns):
            axis = COLOURS[c][0]
            plane_wait(p1[c], layer, agp_s, agp_r, c, False)
            for i in range(plane):
                asm[2 * i:2 * i + 2, base:base + width] = p1[c][layer, i].astype(F32)
            g_buf[c][layer, coord[axis]] = asm[:, base:base + width].astype(BF16)
            own = g_buf[c].at[layer, coord[axis]]
            for d in axis_shifts:
                send(layer, 8 + 3 * c + d - 1, own, own, device(**{axis: d}))
        for i, (_, dst) in enumerate(ffn_pairs):
            recv(layer, 4 + i, dst.at[layer, other], partner)

        across = lax.broadcasted_iota(jnp.int32, (rows, rows), 1)
        down = lax.broadcasted_iota(jnp.int32, (rows, rows), 0)
        parts = []
        for c, (base, width) in enumerate(columns):
            axis = COLOURS[c][0]
            for d in axis_shifts:
                recv(layer, 8 + 3 * c + d - 1, g_buf[c].at[layer, step(coord[axis], side - d)], device(**{axis: d}))
            part = g_buf[c][layer].reshape(rows, width)
            if c:
                pick = (natural_of(down)[c] == across).astype(F32).astype(BF16)
                part = dot(pick, part).astype(BF16)
            parts.append(part)
        g = jnp.concatenate(parts, axis=1)
        hidden = []
        for k in range(2):
            gate = dot_nt(g, wg[layer, k])
            up = dot_nt(g, wu[layer, k])
            hidden.append((jax.nn.silu(gate) * up).astype(BF16))

        for c, (base, width) in enumerate(columns):
            axis = COLOURS[c][0]
            total = None
            for k in range(2):
                a = hidden[k]
                if c:
                    pick = (natural_of(across)[c] == down).astype(F32).astype(BF16)
                    a = dot(pick, a).astype(BF16)
                term = dot(a, wd[layer, k, :, base:base + width])
                total = term if total is None else total + term
            s_buf[c][layer] = total.reshape(side, 2 * plane, width)
            for d in axis_shifts:
                send(layer, 17 + 3 * c + d - 1, s_buf[c].at[layer, step(coord[axis], d)], r1[c].at[layer, d - 1],
                     device(**{axis: d}))
        for c, (base, width) in enumerate(columns):
            axis, a, b = COLOURS[c]
            total = s_buf[c][layer, coord[axis]]
            for d in axis_shifts:
                recv(layer, 17 + 3 * c + d - 1, r1[c].at[layer, d - 1], device(**{axis: d}))
                total = total + r1[c][layer, d - 1]
            for i in range(plane):
                u_buf[c][layer, i] = total[2 * i:2 * i + 2]
            for i, j in plane_shifts:
                target = step(coord[a], i) * side + step(coord[b], j)
                pltpu.make_async_remote_copy(
                    src_ref=u_buf[c].at[layer, target], dst_ref=r2[c].at[layer, slot(c)],
                    send_sem=rsp_s.at[layer, c], recv_sem=rsp_r.at[layer, c],
                    device_id=device(**{a: i, b: j}), device_id_type=MESH).start()
        sums = []
        for c in range(3):
            r2[c][layer, slot(c)] = u_buf[c][layer, slot(c)]
            plane_wait(r2[c], layer, rsp_s, rsp_r, c, False)
            total = r2[c][layer, 0]
            for i in range(1, plane):
                total = total + r2[c][layer, i]
            sums.append(total)
        return (x2 + jnp.concatenate(sums, axis=1)).astype(BF16).astype(F32)

    x2 = xsend[0]
    for layer in range(layers):
        x2 = attention(layer, x2)
        x2 = ffn(layer, x2)
        if layer + 1 < layers:
            xsend[layer + 1] = x2
            send(layer + 1, 0, xsend.at[layer + 1], xrecv.at[layer + 1], partner)
    out_ref[...] = x2
    for copy in pending:
        copy.wait_send()
    for layer in range(layers):
        for c in range(3):
            plane_wait(p1[c], layer, agp_s, agp_r, c, True)
            plane_wait(u_buf[c], layer, rsp_s, rsp_r, c, True)


def solution(mesh):
    devices = mesh.shape['dp']
    side = round((devices // 2) ** (1 / 3))

    def local_step(x, lengths, cache, attn_gain, ffn_gain, w_query, w_attn_out, w_up, w_gate, w_down):
        layers, _, seq, kv = cache.shape
        d_model = x.shape[1]
        heads = w_query.shape[2] // kv
        latent = w_attn_out.shape[1] // heads
        hid = w_up.shape[2]
        hh = heads // 2
        q_chunk, o_chunk = 512, 256
        n_q, n_o = hh * kv // q_chunk, d_model // o_chunk
        plane = side * side
        widths = [w for _, w in colour_columns(d_model)]
        cfg = (side, layers, heads, kv, latent, seq, d_model, q_chunk, o_chunk)
        hbm = pl.BlockSpec(memory_space=pl.ANY)
        scratch = [
            pltpu.VMEM((n_q, d_model, q_chunk), BF16),
            pltpu.VMEM((n_o, hh * latent, o_chunk), BF16),
            pltpu.VMEM((layers, 4, kv, seq), BF16),
            pltpu.VMEM((layers, 2, hid, d_model), BF16),
            pltpu.VMEM((layers, 2, hid, d_model), BF16),
            pltpu.VMEM((layers, 2, hid, d_model), BF16),
            pltpu.VMEM((2, d_model), BF16),
            pltpu.SMEM((2,), jnp.int32),
            pltpu.VMEM((layers, d_model), F32),
            pltpu.VMEM((layers, d_model), F32),
            pltpu.VMEM((2, 2, 128), F32),
            pltpu.VMEM((layers, 2, d_model), F32),
            pltpu.VMEM((layers, 2, d_model), F32),
            pltpu.VMEM((8, hh * kv), F32),
            pltpu.VMEM((4, hh, 640), F32),
            pltpu.VMEM((8, hh * latent), F32),
            pltpu.VMEM((layers, 2, 2, d_model), F32),
            pltpu.VMEM((layers, 2, d_model), F32),
            pltpu.VMEM((2 * plane, d_model), F32),
            *[pltpu.VMEM((layers, plane, 2, w), BF16) for w in widths],
            *[pltpu.VMEM((layers, side, 2 * plane, w), BF16) for w in widths],
            *[pltpu.VMEM((layers, side, 2 * plane, w), F32) for w in widths],
            *[pltpu.VMEM((layers, side - 1, 2 * plane, w), F32) for w in widths],
            *[pltpu.VMEM((layers, plane, 2, w), F32) for w in widths],
            *[pltpu.VMEM((layers, plane, 2, w), F32) for w in widths],
            pltpu.SemaphoreType.DMA((n_q,)),
            pltpu.SemaphoreType.DMA((n_o,)),
            pltpu.SemaphoreType.DMA((layers, 2)),
            pltpu.SemaphoreType.DMA((layers, 3)),
            pltpu.SemaphoreType.DMA((4,)),
            pltpu.SemaphoreType.DMA((layers, 26)),
            pltpu.SemaphoreType.DMA((layers, 26)),
            *[pltpu.SemaphoreType.DMA((layers, 3)) for _ in range(4)],
        ]
        out = pl.pallas_call(
            functools.partial(kernel, cfg),
            out_shape=pltpu.VMEM(x.shape, F32),
            in_specs=[hbm] * 10,
            out_specs=pl.BlockSpec(memory_space=pltpu.VMEM),
            scratch_shapes=scratch,
            compiler_params=pltpu.CompilerParams(
                collective_id=0, has_side_effects=True, vmem_limit_bytes=66_500_000),
            name='mla_decode',
        )(x, lengths, attn_gain, ffn_gain, jnp.swapaxes(cache, 2, 3), w_query, w_attn_out,
          jnp.swapaxes(w_up, 1, 2), jnp.swapaxes(w_gate, 1, 2), w_down)
        return out.astype(BF16)

    rows = ('replica', 'dp')
    return jax.shard_map(
        local_step,
        mesh=mesh,
        in_specs=(P(rows, None), P(rows), P(None, rows, None, None), P(), P(), P(), P(),
                  P(None, None, 'dp'), P(None, None, 'dp'), P(None, 'dp', None)),
        out_specs=P(rows, None),
        check_vma=False,
    )
```

```python
import functools

import jax
import jax.numpy as jnp
from jax import lax
from jax.experimental import pallas as pl
from jax.experimental.pallas import tpu as pltpu
from jax.sharding import PartitionSpec as P

NORM_EPS = 1e-6
MESH = pl.DeviceIdType.MESH
F32 = jnp.float32
BF16 = jnp.bfloat16
COLOURS = (('z', 'y', 'x'), ('x', 'z', 'y'), ('y', 'z', 'x'))


def dot(a, b):
    return jnp.dot(a, b, preferred_element_type=F32)


def dot_nt(a, b):
    return lax.dot_general(a, b, (((1,), (1,)), ((), ())), preferred_element_type=F32)


def colour_columns(d_model):
    tiles = d_model // 128
    widths = [128 * ((tiles + 2 - c) // 3) for c in range(3)]
    return [(sum(widths[:c]), widths[c]) for c in range(3)]


def kernel(
    cfg,
    x_hbm, len_hbm, ag_hbm, fg_hbm, cache_hbm, wq_hbm, wo_hbm, wu_hbm, wg_hbm, wd_hbm,
    out_ref,
    wq, wo, cbuf, wu, wg, wd,
    xin, lens, ag, fg, xsend, xrecv, qrow, qsend, qbuf, obuf, osend, orecv, lhs, ysend, yrecv, asm,
    p1a, p1b, p1c, g_a, g_b, g_c, s_a, s_b, s_c, r1a, r1b, r1c, u_a, u_b, u_c, r2a, r2b, r2c,
    wq_sem, wo_sem, c_sem, f_sem, in_sem, ssem, rsem, agp_s, agp_r, rsp_s, rsp_r,
):
    side, layers, heads, kv, latent, seq, d_model, q_chunk, o_chunk = cfg
    heads_half = heads // 2
    qw = heads_half * kv
    n_q = qw // q_chunk
    n_o = d_model // o_chunk
    kdim = heads_half * latent
    early = n_o - 3
    plane = side * side
    rows = 2 * side ** 3
    scale = (3 * (kv - latent)) ** -0.5
    columns = colour_columns(d_model)
    p1, g_buf, s_buf = (p1a, p1b, p1c), (g_a, g_b, g_c), (s_a, s_b, s_c)
    r1, u_buf, r2 = (r1a, r1b, r1c), (u_a, u_b, u_c), (r2a, r2b, r2c)

    me = lax.axis_index('dp')
    core = lax.rem(me, 2)
    chip = lax.div(me, 2)
    coord = {'x': lax.rem(chip, side), 'y': lax.rem(lax.div(chip, side), side), 'z': lax.div(chip, plane)}
    other = 1 - core

    def step(c, d):
        return lax.rem(c + d, side)

    def device(k=core, **shift):
        at = {a: step(coord[a], shift.get(a, 0)) for a in 'zyx'}
        return {'dp': ((at['z'] * side + at['y']) * side + at['x']) * 2 + k}

    partner = {'dp': chip * 2 + other}
    hops = lambda d: min(d, side - d)
    axis_shifts = sorted(range(1, side), key=hops, reverse=True)
    plane_shifts = sorted(
        [(i, j) for i in range(side) for j in range(side) if i or j],
        key=lambda s: hops(s[0]) + hops(s[1]), reverse=True)

    def wq_copy(layer, i):
        cols = pl.ds(pl.multiple_of(core * qw + i * q_chunk, 128), q_chunk)
        return pltpu.make_async_copy(wq_hbm.at[layer, :, cols], wq.at[i], wq_sem.at[i])

    def wo_copy(layer, i):
        depth = pl.ds(pl.multiple_of(core * kdim, 128), kdim)
        cols = pl.ds(pl.multiple_of(i * o_chunk, 128), o_chunk)
        return pltpu.make_async_copy(wo_hbm.at[layer, depth, cols], wo.at[i], wo_sem.at[i])

    def cache_copy(layer, b):
        return pltpu.make_async_copy(cache_hbm.at[layer, b], cbuf.at[layer, b], c_sem.at[layer, b])

    ffn_pairs = ((wg_hbm, wg), (wu_hbm, wu), (wd_hbm, wd))

    def ffn_copies(layer):
        return [
            pltpu.make_async_copy(src.at[layer], dst.at[layer, core], f_sem.at[layer, i])
            for i, (src, dst) in enumerate(ffn_pairs)]

    inputs = [
        pltpu.make_async_copy(src, dst, in_sem.at[i])
        for i, (src, dst) in enumerate(((x_hbm, xin), (len_hbm, lens), (ag_hbm, ag), (fg_hbm, fg)))]
    for copy in inputs:
        copy.start()
    for i in range(n_q):
        wq_copy(0, i).start()
    for b in range(2):
        cache_copy(0, b).start()

    barrier = pltpu.get_barrier_semaphore()
    peers = [partner] + [
        device(**shift) for shift in
        [{a: d} for a in 'zyx' for d in range(1, side)]
        + [{a: d, b: e} for a, b in ('zy', 'zx', 'yx') for d in range(1, side) for e in range(1, side)]]
    for peer in peers:
        pl.semaphore_signal(barrier, inc=1, device_id=peer, device_id_type=MESH)
    pl.semaphore_wait(barrier, len(peers))

    pending = []

    def remote(layer, index, src, dst, peer):
        return pltpu.make_async_remote_copy(
            src_ref=src, dst_ref=dst, send_sem=ssem.at[layer, index], recv_sem=rsem.at[layer, index],
            device_id=peer, device_id_type=MESH)

    def send(layer, index, src, dst, peer):
        copy = remote(layer, index, src, dst, peer)
        copy.start()
        pending.append(copy)

    def recv(layer, index, dst, peer):
        remote(layer, index, dst, dst, peer).wait_recv()

    def send_ffn(layer, which):
        for i in which:
            src, dst = ffn_pairs[i]
            send(layer, 4 + i, src.at[layer], dst.at[layer, core], partner)

    for copy in inputs:
        copy.wait()
    xsend[0] = xin[...].astype(F32)
    send(0, 0, xsend.at[0], xrecv.at[0], partner)
    send_ffn(0, (0, 1))
    lhs[4:8, :] = jnp.zeros((4, kdim), F32)

    def rms(v, gain):
        mean_sq = jnp.mean(v * v, axis=-1, keepdims=True)
        return v * lax.rsqrt(mean_sq + NORM_EPS) * gain

    def attention(layer, x2):
        recv(layer, 0, xrecv.at[layer], partner)
        x4 = jnp.concatenate([x2, xrecv[layer]], axis=0)
        normed = rms(x4, ag[layer:layer + 1, :])
        h8 = jnp.concatenate([normed, normed], axis=0).astype(BF16)

        def q_step(i, carry):
            wq_copy(layer, i).wait()
            if layer == 0:
                @pl.when(i < early)
                def _():
                    wo_copy(layer, i).start()
            qrow[:, pl.ds(pl.multiple_of(i * q_chunk, 128), q_chunk)] = dot(h8, wq[i])
            return carry

        lax.fori_loop(0, n_q, q_step, 0)
        pair = 2 * kv
        for j in range(heads_half // 2):
            block = qrow[:, j * pair:(j + 1) * pair]
            odd = pltpu.roll(block[:, latent:latent + 640], 640 - 64, 1)
            for parity, q8 in ((0, block[:, :640]), (1, odd)):
                h = 2 * j + parity
                for b in range(2):
                    qbuf[layer, core, b, h:h + 1, :] = q8[b:b + 1, :]
                    qsend[layer, b, h:h + 1, :] = q8[2 + b:3 + b, :]
        send(layer, 2, qsend.at[layer], qbuf.at[layer, core], partner)
        if layer == 0:
            wo_copy(layer, early).start()
        positions = lax.broadcasted_iota(jnp.int32, (heads, seq), 1)
        for b in range(2):
            cache_copy(layer, b).wait()
        recv(layer, 2, qbuf.at[layer, other], partner)
        for b in range(2):
            q = jnp.concatenate([qbuf[layer, 0, b], qbuf[layer, 1, b]], axis=0)[:, :kv].astype(BF16)
            s = dot(q, cbuf[layer, b]) * scale
            s = jnp.where(positions < lens[b], s, -jnp.inf)
            e = jnp.exp(s - jnp.max(s, axis=-1, keepdims=True))
            p = (e / jnp.sum(e, axis=-1, keepdims=True)).astype(BF16)
            o = dot_nt(p, cbuf[layer, b, :latent, :])
            obuf[b, 0] = o[:heads_half]
            obuf[b, 1] = o[heads_half:]
            if layer == 0:
                wo_copy(layer, early + 1 + b).start()
        if layer == 0:
            for copy in ffn_copies(layer):
                copy.start()
        for b in range(2):
            theirs = obuf[b, other]
            for h in range(heads_half):
                osend[layer, b:b + 1, h * latent:(h + 1) * latent] = theirs[h:h + 1, :]
        send(layer, 3, osend.at[layer], orecv.at[layer], partner)
        for b in range(2):
            mine = obuf[b, core]
            for h in range(heads_half):
                lhs[b:b + 1, h * latent:(h + 1) * latent] = mine[h:h + 1, :]
        recv(layer, 3, orecv.at[layer], partner)
        lhs[2:4, :] = orecv[layer]
        lhs_b = lhs[...].astype(BF16)

        def o_step(i, carry):
            wo_copy(layer, i).wait()
            y = dot(lhs_b, wo[i])
            cols = pl.ds(pl.multiple_of(i * o_chunk, 128), o_chunk)
            ysend[layer, 0, :, cols] = y[0:2]
            ysend[layer, 1, :, cols] = y[2:4]
            return carry

        lax.fori_loop(0, n_o, o_step, 0)
        send(layer, 1, ysend.at[layer, 1], yrecv.at[layer], partner)
        for copy in ffn_copies(layer):
            copy.wait()
        if layer == 0:
            send_ffn(0, (2,))
        if layer + 1 < layers:
            for b in range(2):
                cache_copy(layer + 1, b).start()
            for copy in ffn_copies(layer + 1):
                copy.start()
            for i in range(n_q):
                wq_copy(layer + 1, i).start()
            for i in range(n_o):
                wo_copy(layer + 1, i).start()
        recv(layer, 1, yrecv.at[layer], partner)
        return (x2 + (ysend[layer, 0] + yrecv[layer])).astype(BF16).astype(F32)

    def slot(c):
        _, a, b = COLOURS[c]
        return coord[a] * side + coord[b]

    def plane_wait(buf, layer, send_sem, recv_sem, c, sent):
        part = buf.at[layer, pl.ds(0, plane - 1)]
        copy = pltpu.make_async_remote_copy(
            src_ref=part, dst_ref=part, send_sem=send_sem.at[layer, c], recv_sem=recv_sem.at[layer, c],
            device_id=partner, device_id_type=MESH)
        return copy.wait_send() if sent else copy.wait_recv()

    def natural_of(index):
        log = side.bit_length() - 1
        r = index & 1
        at = {'x': (index >> 1) & (side - 1), 'y': (index >> (1 + log)) & (side - 1), 'z': index >> (1 + 2 * log)}
        return [
            (((at[o] << (2 * log)) | (at[a] << log) | at[b]) << 1) | r for o, a, b in COLOURS]

    def ffn(layer, x2):
        g2 = rms(x2, fg[layer:layer + 1, :]).astype(BF16)
        for c, (base, width) in enumerate(columns):
            _, a, b = COLOURS[c]
            p1[c][layer, slot(c)] = g2[:, base:base + width]
            for i, j in plane_shifts:
                block = p1[c].at[layer, slot(c)]
                pltpu.make_async_remote_copy(
                    src_ref=block, dst_ref=block, send_sem=agp_s.at[layer, c], recv_sem=agp_r.at[layer, c],
                    device_id=device(**{a: i, b: j}), device_id_type=MESH).start()
        if layer + 1 < layers:
            send_ffn(layer + 1, (0, 1, 2))
        for c, (base, width) in enumerate(columns):
            axis = COLOURS[c][0]
            plane_wait(p1[c], layer, agp_s, agp_r, c, False)
            for i in range(plane):
                asm[2 * i:2 * i + 2, base:base + width] = p1[c][layer, i].astype(F32)
            g_buf[c][layer, coord[axis]] = asm[:, base:base + width].astype(BF16)
            own = g_buf[c].at[layer, coord[axis]]
            for d in axis_shifts:
                send(layer, 8 + 3 * c + d - 1, own, own, device(**{axis: d}))
        for i, (_, dst) in enumerate(ffn_pairs):
            recv(layer, 4 + i, dst.at[layer, other], partner)

        across = lax.broadcasted_iota(jnp.int32, (rows, rows), 1)
        down = lax.broadcasted_iota(jnp.int32, (rows, rows), 0)
        parts = []
        for c, (base, width) in enumerate(columns):
            axis = COLOURS[c][0]
            for d in axis_shifts:
                recv(layer, 8 + 3 * c + d - 1, g_buf[c].at[layer, step(coord[axis], side - d)], device(**{axis: d}))
            part = g_buf[c][layer].reshape(rows, width)
            if c:
                pick = (natural_of(down)[c] == across).astype(F32).astype(BF16)
                part = dot(pick, part).astype(BF16)
            parts.append(part)
        g = jnp.concatenate(parts, axis=1)
        hidden = []
        for k in range(2):
            gate = dot_nt(g, wg[layer, k])
            up = dot_nt(g, wu[layer, k])
            hidden.append((jax.nn.silu(gate) * up).astype(BF16))

        for c, (base, width) in enumerate(columns):
            axis = COLOURS[c][0]
            total = None
            for k in range(2):
                a = hidden[k]
                if c:
                    pick = (natural_of(across)[c] == down).astype(F32).astype(BF16)
                    a = dot(pick, a).astype(BF16)
                term = dot(a, wd[layer, k, :, base:base + width])
                total = term if total is None else total + term
            s_buf[c][layer] = total.reshape(side, 2 * plane, width)
            for d in axis_shifts:
                send(layer, 17 + 3 * c + d - 1, s_buf[c].at[layer, step(coord[axis], d)], r1[c].at[layer, d - 1],
                     device(**{axis: d}))
        for c, (base, width) in enumerate(columns):
            axis, a, b = COLOURS[c]
            total = s_buf[c][layer, coord[axis]]
            for d in axis_shifts:
                recv(layer, 17 + 3 * c + d - 1, r1[c].at[layer, d - 1], device(**{axis: d}))
                total = total + r1[c][layer, d - 1]
            for i in range(plane):
                u_buf[c][layer, i] = total[2 * i:2 * i + 2]
            for i, j in plane_shifts:
                target = step(coord[a], i) * side + step(coord[b], j)
                pltpu.make_async_remote_copy(
                    src_ref=u_buf[c].at[layer, target], dst_ref=r2[c].at[layer, slot(c)],
                    send_sem=rsp_s.at[layer, c], recv_sem=rsp_r.at[layer, c],
                    device_id=device(**{a: i, b: j}), device_id_type=MESH).start()
        sums = []
        for c in range(3):
            r2[c][layer, slot(c)] = u_buf[c][layer, slot(c)]
            plane_wait(r2[c], layer, rsp_s, rsp_r, c, False)
            total = r2[c][layer, 0]
            for i in range(1, plane):
                total = total + r2[c][layer, i]
            sums.append(total)
        return (x2 + jnp.concatenate(sums, axis=1)).astype(BF16).astype(F32)

    x2 = xsend[0]
    for layer in range(layers):
        x2 = attention(layer, x2)
        x2 = ffn(layer, x2)
        if layer + 1 < layers:
            xsend[layer + 1] = x2
            send(layer + 1, 0, xsend.at[layer + 1], xrecv.at[layer + 1], partner)
    out_ref[...] = x2
    for copy in pending:
        copy.wait_send()
    for layer in range(layers):
        for c in range(3):
            plane_wait(p1[c], layer, agp_s, agp_r, c, True)
            plane_wait(u_buf[c], layer, rsp_s, rsp_r, c, True)


def solution(mesh):
    devices = mesh.shape['dp']
    side = round((devices // 2) ** (1 / 3))

    def local_step(x, lengths, cache, attn_gain, ffn_gain, w_query, w_attn_out, w_up, w_gate, w_down):
        layers, _, seq, kv = cache.shape
        d_model = x.shape[1]
        heads = w_query.shape[2] // kv
        latent = w_attn_out.shape[1] // heads
        hid = w_up.shape[2]
        hh = heads // 2
        q_chunk, o_chunk = 512, 256
        n_q, n_o = hh * kv // q_chunk, d_model // o_chunk
        plane = side * side
        widths = [w for _, w in colour_columns(d_model)]
        cfg = (side, layers, heads, kv, latent, seq, d_model, q_chunk, o_chunk)
        hbm = pl.BlockSpec(memory_space=pl.ANY)
        scratch = [
            pltpu.VMEM((n_q, d_model, q_chunk), BF16),
            pltpu.VMEM((n_o, hh * latent, o_chunk), BF16),
            pltpu.VMEM((layers, 2, kv, seq), BF16),
            pltpu.VMEM((layers, 2, hid, d_model), BF16),
            pltpu.VMEM((layers, 2, hid, d_model), BF16),
            pltpu.VMEM((layers, 2, hid, d_model), BF16),
            pltpu.VMEM((2, d_model), BF16),
            pltpu.SMEM((2,), jnp.int32),
            pltpu.VMEM((layers, d_model), F32),
            pltpu.VMEM((layers, d_model), F32),
            pltpu.VMEM((layers, 2, d_model), F32),
            pltpu.VMEM((layers, 2, d_model), F32),
            pltpu.VMEM((8, hh * kv), F32),
            pltpu.VMEM((layers, 2, hh, 640), F32),
            pltpu.VMEM((layers, 2, 2, hh, 640), F32),
            pltpu.VMEM((2, 2, hh, latent), F32),
            pltpu.VMEM((layers, 2, hh * latent), F32),
            pltpu.VMEM((layers, 2, hh * latent), F32),
            pltpu.VMEM((8, hh * latent), F32),
            pltpu.VMEM((layers, 2, 2, d_model), F32),
            pltpu.VMEM((layers, 2, d_model), F32),
            pltpu.VMEM((2 * plane, d_model), F32),
            *[pltpu.VMEM((layers, plane, 2, w), BF16) for w in widths],
            *[pltpu.VMEM((layers, side, 2 * plane, w), BF16) for w in widths],
            *[pltpu.VMEM((layers, side, 2 * plane, w), F32) for w in widths],
            *[pltpu.VMEM((layers, side - 1, 2 * plane, w), F32) for w in widths],
            *[pltpu.VMEM((layers, plane, 2, w), F32) for w in widths],
            *[pltpu.VMEM((layers, plane, 2, w), F32) for w in widths],
            pltpu.SemaphoreType.DMA((n_q,)),
            pltpu.SemaphoreType.DMA((n_o,)),
            pltpu.SemaphoreType.DMA((layers, 2)),
            pltpu.SemaphoreType.DMA((layers, 3)),
            pltpu.SemaphoreType.DMA((4,)),
            pltpu.SemaphoreType.DMA((layers, 26)),
            pltpu.SemaphoreType.DMA((layers, 26)),
            *[pltpu.SemaphoreType.DMA((layers, 3)) for _ in range(4)],
        ]
        out = pl.pallas_call(
            functools.partial(kernel, cfg),
            out_shape=pltpu.VMEM(x.shape, F32),
            in_specs=[hbm] * 10,
            out_specs=pl.BlockSpec(memory_space=pltpu.VMEM),
            scratch_shapes=scratch,
            compiler_params=pltpu.CompilerParams(
                collective_id=0, has_side_effects=True, vmem_limit_bytes=66_500_000),
            name='mla_decode',
        )(x, lengths, attn_gain, ffn_gain, jnp.swapaxes(cache, 2, 3), w_query, w_attn_out,
          jnp.swapaxes(w_up, 1, 2), jnp.swapaxes(w_gate, 1, 2), w_down)
        return out.astype(BF16)

    rows = ('replica', 'dp')
    return jax.shard_map(
        local_step,
        mesh=mesh,
        in_specs=(P(rows, None), P(rows), P(None, rows, None, None), P(), P(), P(), P(),
                  P(None, None, 'dp'), P(None, None, 'dp'), P(None, 'dp', None)),
        out_specs=P(rows, None),
        check_vma=False,
    )
```
